32 devices in a mesh: section: 4 (over x, core), fsdp: 8 (over z, y).
Axes of the slice: x: 2, y: 2, z: 4, core: 2. Of those that a mesh axis runs over, the one named last changes fastest.
Arguments:
- tokens: bfloat16 [4, 2, 1024, 8192], P('section', None, 'fsdp'), may hold values from -6 to 6
- queries: bfloat16 [4, 2, 1024, 4096], P('section', None, 'fsdp'), may hold values from -200 to 200
- gains: bfloat16 [4, 8192], P('section'), may hold values from 0.5 to 1.5
- key_weight: bfloat16 [4, 8192, 512], P('section', 'fsdp'), may hold values from -0.0625 to 0.0625
- value_weight: bfloat16 [4, 8192, 512], P('section', 'fsdp'), may hold values from -0.0625 to 0.0625
- lengths: int32 [2, 16], replicated, may hold values from 1 to 128, 1024 in all within a row
Outputs:
- attended: bfloat16 [4, 2, 1024, 4096], P('section', None, 'fsdp')
The draws below stay inside these ranges and needn't reach their ends.
Inputs may be any that keep to these rules, and one draw needn't show every extreme that they name: `lengths`: each row sums to 1024; some document has exactly 128 tokens.
All inputs are finite; a program needn't handle non-finite values.
Results may differ from the reference program's by a relative error of at most 0.012.
The reference program's roundings to bfloat16 on the way (of `normed`) count: a program that leaves them out, or rounds other values in their place, can miss the bound.
Values may be sent and summed in bfloat16 or wider, within the bound.
A program may use at most 128 MiB of HBM per device.

```python
import math
import jax
import jax.numpy as jnp
import numpy as np
from jax import lax

D = 8192
KV_HEADS = 4
Q_HEADS = 32
HEAD = 128
MICRO = 2
TOK_DEV = 128
TOKENS = 1024
DOCS = 16
LAYERS = 4


def draw_queries(key, part):
    shape = (LAYERS, MICRO, TOKENS, Q_HEADS * HEAD)
    normal_part = jax.random.normal(jax.random.fold_in(key, 11), shape, jnp.float32)
    drawn = jnp.clip(normal_part, -6.0, 6.0)
    return drawn.astype(jnp.bfloat16)


def block_levels(stream_key, extent, pieces, low, high):
    def one(position, blocks):
        draws = jax.random.uniform(jax.random.fold_in(jax.random.fold_in(stream_key, 6), position), (blocks,), jnp.float32, low / len(pieces), high / len(pieces))
        return jnp.repeat(jnp.exp(draws), extent[position] // blocks).reshape((-1,) + (1,) * (len(extent) - position - 1))

    factor_of = one(*pieces[0])
    for cut in pieces[1:]:
        factor_of = factor_of * one(*cut)
    return factor_of


def profile(number_of, total, most, skew):
    portions = [(1 << 20) // math.isqrt(standing ** skew) + 1 for standing in range(2, number_of + 1)]
    spare, holding = total - most - (number_of - 1), [1] * (number_of - 1)
    while spare > 0:
        movable = [i for i in range(number_of - 1) if holding[i] < most]
        mass, remaining = sum([portions[i] for i in movable]), spare
        for i in movable:
            addition = min(most - holding[i], max(1, remaining * portions[i] // mass), spare)
            holding[i] = holding[i] + addition
            spare = spare - addition
    return np.array([most] + holding)


def ragged_sizes(rng, amount, total, most, slope):
    if amount == 2:
        one = jax.random.randint(rng, (), max(1, total - most), min(most, total - 1) + 1)
        return jnp.stack([one, total - one])
    sizes = jnp.asarray(profile(amount, total, most, slope), jnp.int32)
    couples = (amount - 1) // 2
    source_of, taker = sizes[1:1 + 2 * couples:2], sizes[2:2 + 2 * couples:2]
    room = jnp.minimum(source_of - 1, most - taker)
    passed = jax.random.randint(jax.random.fold_in(rng, 1), (couples,), 0, 1 << 20) % (room + 1)
    sizes = sizes.at[1:1 + 2 * couples:2].set(source_of - passed).at[2:2 + 2 * couples:2].set(taker + passed)
    return sizes[jax.random.permutation(jax.random.fold_in(rng, 2), amount)]


def scatter_about(own_key, dims, width, most, pieces=(), kind=jnp.bfloat16):
    values = jax.random.normal(own_key, dims, jnp.float32) * width
    if len(pieces) > 0:
        values = block_levels(own_key, dims, pieces, -0.22, 0.18) * values
    return jnp.clip(values, min=-most, max=most).astype(kind)


def setup_inputs(seed: int = 0) -> dict:
    key_list = jax.random.split(jax.random.key(seed), 7)
    return {
        "tokens": scatter_about(key_list[0], (LAYERS, MICRO, TOKENS, D), 1.0, 6.0, ((0, 4), (2, 8))),
        "queries": draw_queries(jax.random.fold_in(key_list[6], 71), 0),
        "gains": jnp.clip(1.0 + 0.1 * jax.random.normal(key_list[2], (LAYERS, D), jnp.float32), 0.5, 1.5).astype(jnp.bfloat16),
        "key_weight": scatter_about(key_list[3], (LAYERS, D, KV_HEADS * HEAD), D ** -0.5, 0.0625, ((0, 4), (1, 8))),
        "value_weight": scatter_about(key_list[4], (LAYERS, D, KV_HEADS * HEAD), D ** -0.5, 0.0625, ((0, 4), (1, 8))),
        "lengths": jax.vmap(lambda own: ragged_sizes(own, DOCS, TOKENS, TOK_DEV, 2))(jax.random.split(key_list[5], MICRO)).reshape((MICRO, DOCS)).astype(jnp.int32),
    }


def rms_norm(hidden, gain_row):
    widened = hidden.astype(jnp.float32)
    inverse_rms = lax.rsqrt(lax.optimization_barrier(jnp.mean(widened * widened, axis=-1, keepdims=True)) + 1e-05)
    return (widened * inverse_rms * gain_row.astype(jnp.float32)).astype(jnp.bfloat16)

def document_ids(length_row, positions):
    bounds = jnp.cumsum(length_row.astype(jnp.int32))
    return lax.optimization_barrier(jnp.sum((bounds[None, :] <= positions[:, None]).astype(jnp.int32), axis=1))

def block_attend(query_rows, key_rows, value_rows, query_pos, key_pos, query_doc, key_doc):
    query_count = query_rows.shape[0]
    key_count = key_rows.shape[0]
    kv_count = key_rows.shape[1] // HEAD
    group_count = query_rows.shape[1] // (kv_count * HEAD)
    query_heads = query_rows.reshape(query_count, kv_count, group_count, HEAD).astype(jnp.float32)
    key_heads = key_rows.reshape(key_count, kv_count, HEAD).astype(jnp.float32)
    value_heads = value_rows.reshape(key_count, kv_count, HEAD).astype(jnp.float32)
    scores = jnp.einsum('tkgd,skd->kgts', query_heads, key_heads) * HEAD ** (-0.5)
    allowed = (key_doc[None, :] == query_doc[:, None]) & (key_pos[None, :] <= query_pos[:, None]) & (key_pos[None, :] >= 0)
    scores = jnp.where(allowed, scores, -1e+30)
    maxima = lax.optimization_barrier(jnp.max(scores, axis=-1, keepdims=True))
    exponent = jnp.where(allowed, jnp.exp(scores - maxima), 0.0)
    totals = lax.optimization_barrier(jnp.sum(exponent, axis=-1, keepdims=True))
    softmax_rows = (exponent / totals).astype(jnp.bfloat16)
    mixed = jnp.einsum('kgts,skd->tkgd', softmax_rows.astype(jnp.float32), value_heads)
    return mixed.reshape(query_count, kv_count * group_count * HEAD).astype(jnp.bfloat16)

def attend_all(query_all, key_all, value_all, length_row):
    block_count = TOKENS // TOK_DEV
    zero_rows = jnp.zeros((TOK_DEV, key_all.shape[1]), jnp.bfloat16)
    padded_keys = jnp.concatenate([zero_rows, key_all], axis=0)
    padded_values = jnp.concatenate([zero_rows, value_all], axis=0)

    def attend_block(block_index):
        block_start = (block_index * TOK_DEV).astype(jnp.int32)
        query_rows = lax.dynamic_slice_in_dim(query_all, block_start, TOK_DEV, 0)
        key_rows = lax.dynamic_slice_in_dim(padded_keys, block_start, 2 * TOK_DEV, 0)
        value_rows = lax.dynamic_slice_in_dim(padded_values, block_start, 2 * TOK_DEV, 0)
        query_pos = block_start + jnp.arange(TOK_DEV, dtype=jnp.int32)
        key_pos = block_start - TOK_DEV + jnp.arange(2 * TOK_DEV, dtype=jnp.int32)
        return block_attend(query_rows, key_rows, value_rows, query_pos, key_pos, document_ids(length_row, query_pos), document_ids(length_row, key_pos))
    blocks_out = lax.map(attend_block, jnp.arange(block_count, dtype=jnp.int32))
    return blocks_out.reshape(TOKENS, query_all.shape[1])

def reference(tokens, queries, gains, key_weight, value_weight, lengths):
    results = []
    for slot_index in range(MICRO):
        per_layer = []
        for layer_index in range(LAYERS):
            normed = rms_norm(tokens[layer_index, slot_index], gains[layer_index])
            key_all = jnp.dot(normed, key_weight[layer_index], preferred_element_type=jnp.float32).astype(jnp.bfloat16)
            value_all = jnp.dot(normed, value_weight[layer_index], preferred_element_type=jnp.float32).astype(jnp.bfloat16)
            per_layer.append(attend_all(queries[layer_index, slot_index], key_all, value_all, lengths[slot_index]))
        results.append(jnp.stack(per_layer))
    return jnp.stack(results, axis=1)
```

```python
import functools

import jax
import jax.numpy as jnp
from jax import lax
from jax.experimental import pallas as pl
from jax.experimental.pallas import tpu as pltpu
from jax.sharding import PartitionSpec as P

HEAD = 128
AXIS = "fsdp"
LEAD = 2


def kernel(
    n, keep,
    x_hbm, q_hbm, gain_ref, kw_hbm, vw_hbm, len_ref, o_hbm,
    x_v, q_v, o_v, wbuf, xs, sx, lx, acc, zs, zr, ys, yr, kv, prior, start_s,
    lw_sem, lx_sem, lq_sem, lo_sem,
    wz_s, wz_r, wh_s, wh_r, wk_s, wk_r, xy_s, xy_r, xz_s, xz_r,
    z_s, z_r, y_s, y_r, p_s, p_r,
):
    slots, tok, depth = x_v.shape
    pieces, groups, _, rows, _ = wbuf.shape
    heads = pieces // 2
    total = slots * tok
    q_per_kv = q_v.shape[2] // (heads * HEAD)
    me = lax.axis_index(AXIS)
    bit = me % 2
    cls = (me // 2) % 2
    grp = me // 4
    leaf = cls == grp % 2
    hub = jnp.logical_not(leaf)
    kind = jnp.where(leaf, 1, 0)
    y_peer = me + 1 - 2 * bit
    z_peer = me + 2 - 4 * cls
    right = lax.rem(me + 1, n)
    left = lax.rem(me + n - 1, n)
    others = [lax.rem(grp + d, groups) for d in range(1, groups)]
    span = range(len(others))

    def hub_of(g):
        return 4 * g + 2 * (1 - g % 2) + bit

    def load_w(j):
        w = vw_hbm if j % 2 else kw_hbm
        cols = pl.ds((j // 2) * HEAD, HEAD)
        return pltpu.make_async_copy(w.at[0, :, cols], wbuf.at[j, grp, kind], lw_sem.at[j])

    x_loads = [pltpu.make_async_copy(x_hbm.at[0, s], x_v.at[s], lx_sem.at[s]) for s in range(slots)]
    q_load = pltpu.make_async_copy(q_hbm.at[0], q_v, lq_sem)
    w_loads = [load_w(j) for j in range(pieces)]
    for copy in w_loads[:2] + x_loads[:1] + w_loads[2:] + x_loads[1:] + [q_load]:
        copy.start()

    barrier = pltpu.get_barrier_semaphore()

    def greet(peer):
        pl.semaphore_signal(barrier, inc=1, device_id={AXIS: peer}, device_id_type=pl.DeviceIdType.MESH)

    greet(y_peer)
    greet(z_peer)

    @pl.when(hub)
    def _():
        for g in others:
            greet(hub_of(g))

    @pl.when(me < n - 1)
    def _():
        greet(right)

    @pl.when(me > 0)
    def _():
        greet(left)

    prior[...] = jnp.zeros_like(prior)
    pl.semaphore_wait(
        barrier,
        2 + jnp.where(hub, len(others), 0) + jnp.where(me < n - 1, 1, 0) + jnp.where(me > 0, 1, 0),
    )

    def remote(src, dst, send, recv, peer):
        return pltpu.make_async_remote_copy(
            src_ref=src, dst_ref=dst, send_sem=send, recv_sem=recv,
            device_id={AXIS: peer}, device_id_type=pl.DeviceIdType.MESH,
        )

    def w_pair(j, k):
        block = wbuf.at[j, grp, k]
        return remote(block, block, wz_s.at[j], wz_r.at[j], z_peer)

    def w_hub(j, k, d, g):
        block = wbuf.at[j, g, k]
        return remote(block, block, wh_s.at[j, k, d], wh_r.at[j, k, g], hub_of(others[d]))

    def w_keep(j, d):
        block = wbuf.at[j, others[d], 0, pl.ds(0, keep)]
        return remote(block, block, wk_s.at[j, d], wk_r.at[j, d], z_peer)

    def x_y(s, g, k):
        return remote(
            sx.at[g, k, pl.ds(s * tok, tok)], xs.at[g, k, pl.ds(total + s * tok, tok)],
            xy_s.at[s, g, k], xy_r.at[s, g, k], y_peer,
        )

    def x_z(p, d, k):
        skip = 0 if k else keep
        here = (others[d], k, pl.ds(p * tok, tok), pl.ds(skip, rows - skip))
        return remote(xs.at[here], lx.at[here], xz_s.at[p, d, k], xz_r.at[p, d, k], z_peer)

    def z_copy(j):
        return remote(zs.at[j], zr.at[j], z_s.at[j], z_r.at[j], z_peer)

    def y_copy(j):
        return remote(ys.at[j], yr.at[j], y_s.at[j], y_r.at[j], y_peer)

    def p_copy(j):
        return remote(kv.at[j], prior.at[j], p_s.at[j], p_r.at[j], right)

    for j in range(pieces):
        w_loads[j].wait()

        @pl.when(hub)
        def _(j=j):
            w_pair(j, 0).start()
            for d in span:
                w_hub(j, 0, d, grp).start()

        if j < LEAD:
            @pl.when(leaf)
            def _(j=j):
                w_pair(j, 1).start()

    block_rows = 16

    def norm_block(s, r):
        here = pl.ds(pl.multiple_of(r * block_rows, block_rows), block_rows)
        there = pl.ds(pl.multiple_of(s * tok + r * block_rows, block_rows), block_rows)
        squares = jnp.zeros((block_rows, 1), jnp.float32)
        step = 4 * HEAD
        for i in range(depth // step):
            piece = x_v[s, here, i * step:(i + 1) * step].astype(jnp.float32)
            squares = squares + jnp.sum(piece * piece, axis=-1, keepdims=True)
        inverse = lax.rsqrt(squares / depth + 1e-05)
        for g in range(groups):
            for k in range(2):
                line = g % 2 if k else 1 - g % 2
                for mine in (False, True):
                    first = (4 * g + 2 * line + (bit if mine else 1 - bit)) * rows
                    cols = pl.ds(pl.multiple_of(first, HEAD), rows)
                    value = x_v[s, here, cols].astype(jnp.float32) * inverse
                    value = (value * gain_ref[0:1, cols].astype(jnp.float32)).astype(jnp.bfloat16)
                    if mine:
                        xs[g, k, there, :] = value
                    else:
                        sx[g, k, there, :] = value

    for s in range(slots):
        x_loads[s].wait()

        def norm_step(r, carry, s=s):
            norm_block(s, r)
            return carry

        lax.fori_loop(0, tok // block_rows, norm_step, 0)
        for g in others + [grp]:
            for k in range(2):
                x_y(s, g, k).start()

        @pl.when(leaf)
        def _(s=s):
            for d in span:
                for k in range(2):
                    x_z(s, d, k).start()

    docs = len_ref.shape[1]
    rowi = lax.broadcasted_iota(jnp.int32, (docs, docs), 0)
    coli = lax.broadcasted_iota(jnp.int32, (docs, docs), 1)
    pos = lax.broadcasted_iota(jnp.int32, (tok, 1), 0) + me * tok
    for s in range(slots):
        lens = jnp.broadcast_to(len_ref[s:s + 1, :], (docs, docs))
        bounds = jnp.sum(jnp.where(coli <= rowi, lens, 0), axis=1, keepdims=True)
        bound_row = jnp.sum(jnp.where(coli == rowi, bounds, 0), axis=0, keepdims=True)
        start = jnp.max(jnp.where(bound_row <= pos, bound_row, 0), axis=1, keepdims=True)
        start_s[s] = jnp.broadcast_to(start, (tok, HEAD))
    q_load.wait()

    def dot(a, b):
        return jnp.dot(a, b, preferred_element_type=jnp.float32)

    def loop(lo, hi, step):
        def run(j, carry):
            step(j)
            return carry

        lax.fori_loop(lo, hi, run, 0)

    def take_hub(j):
        for d in span:
            w_hub(j, 0, d, others[d]).wait_recv()
            if keep:
                w_keep(j, d).start()

    def pass_leaf(j):
        w_pair(j, 1).wait_recv()
        for d in span:
            w_hub(j, 1, d, grp).start()

    @pl.when(hub)
    def _():
        loop(0, pieces // 2, take_hub)
        loop(0, LEAD, pass_leaf)
        loop(pieces // 2, pieces, take_hub)
        pass_leaf(LEAD)
        for s in range(slots):
            for g in others + [grp]:
                for k in range(2):
                    x_y(s, g, k).wait_recv()

        def first(j):
            value = dot(xs[grp, 0], wbuf[j, grp, 0])
            for g in others:
                value = value + dot(xs[g, 0], wbuf[j, g, 0])
            acc[j] = value

        loop(0, pieces, first)
        for p in range(2 * slots):
            for d in span:
                for k in range(2):
                    x_z(p, d, k).wait_recv()

    @pl.when(leaf)
    def _():
        for s in range(slots):
            for d in span:
                for k in range(2):
                    x_y(s, others[d], k).wait_recv()
                    x_z(slots + s, d, k).start()

        def send_w(j):
            w_pair(j, 1).start()

        loop(LEAD, pieces, send_w)
        for s in range(slots):
            for k in range(2):
                x_y(s, grp, k).wait_recv()

        def first(j):
            w_pair(j, 0).wait_recv()
            acc[j] = dot(xs[grp, 0], wbuf[j, grp, 0]) + dot(xs[grp, 1], wbuf[j, grp, 1])

        loop(0, pieces, first)
        if keep:
            def second(j):
                value = acc[j]
                for d in span:
                    w_keep(j, d).wait_recv()
                    value = value + dot(
                        xs[others[d], 0, :, 0:keep], wbuf[j, others[d], 0, 0:keep]
                    )
                acc[j] = value

            loop(0, pieces, second)

    def meet(j):
        @pl.when(hub)
        def _():
            for d in span:
                w_hub(j, 1, d, others[d]).wait_recv()
            value = jnp.zeros((2 * total, HEAD), jnp.float32)
            for g in others:
                value = value + dot(lx[g, 0, :, keep:], wbuf[j, g, 0, keep:])
                value = value + dot(lx[g, 1], wbuf[j, g, 1])
            zs[j] = value.astype(jnp.bfloat16)
            z_copy(j).start()
            value = acc[j] + dot(xs[grp, 1], wbuf[j, grp, 1])
            for g in others:
                value = value + dot(xs[g, 1], wbuf[j, g, 1])
            acc[j] = value
            ys[j] = value[total:].astype(jnp.bfloat16)
            y_copy(j).start()

            @pl.when(j + LEAD + 1 < pieces)
            def _():
                pass_leaf(j + LEAD + 1)

        @pl.when(leaf)
        def _():
            z_copy(j).wait_recv()
            value = acc[j] + zr[j].astype(jnp.float32)
            acc[j] = value
            ys[j] = value[total:].astype(jnp.bfloat16)
            y_copy(j).start()

    def finish(j):
        y_copy(j).wait_recv()
        kv[j] = (acc[j, 0:total] + yr[j].astype(jnp.float32)).astype(jnp.bfloat16)

        @pl.when(me < n - 1)
        def _():
            p_copy(j).start()

    key_pos = lax.broadcasted_iota(jnp.int32, (tok, 2 * tok), 1) + (me - 1) * tok
    query_pos = lax.broadcasted_iota(jnp.int32, (tok, 2 * tok), 0) + me * tok
    wide = q_per_kv * HEAD

    def out_copy(h):
        cols = pl.ds(pl.multiple_of(h * wide, HEAD), wide)
        return pltpu.make_async_copy(o_v.at[:, :, cols], o_hbm.at[0, :, :, cols], lo_sem.at[h])

    def attend(h):
        @pl.when(me > 0)
        def _():
            p_copy(2 * h).wait_recv()
            p_copy(2 * h + 1).wait_recv()

        for s in range(slots):
            here = slice(s * tok, (s + 1) * tok)
            keys = jnp.concatenate([prior[2 * h, here], kv[2 * h, here]], axis=0)
            values = jnp.concatenate([prior[2 * h + 1, here], kv[2 * h + 1, here]], axis=0)
            allowed = (key_pos >= start_s[s][:, 0:1]) & (key_pos <= query_pos)
            for q in range(q_per_kv):
                cols = pl.ds(pl.multiple_of((h * q_per_kv + q) * HEAD, HEAD), HEAD)
                scores = lax.dot_general(
                    q_v[s, :, cols], keys, (((1,), (1,)), ((), ())),
                    preferred_element_type=jnp.float32,
                ) * HEAD ** (-0.5)
                scores = jnp.where(allowed, scores, -1e30)
                maxima = jnp.max(scores, axis=-1, keepdims=True)
                exponent = jnp.where(allowed, jnp.exp(scores - maxima), 0.0)
                sums = jnp.sum(exponent, axis=-1, keepdims=True)
                soft = (exponent / sums).astype(jnp.bfloat16)
                o_v[s, :, cols] = dot(soft, values).astype(jnp.bfloat16)
        out_copy(h).start()

    def round_of(h):
        meet(2 * h)
        finish(2 * h)
        meet(2 * h + 1)

        @pl.when(h > 0)
        def _():
            attend(h - 1)

        finish(2 * h + 1)

    loop(0, heads, round_of)
    attend(heads - 1)

    def drain(j):
        y_copy(j).wait_send()

        @pl.when(me < n - 1)
        def _():
            p_copy(j).wait_send()

        @pl.when(hub)
        def _():
            w_pair(j, 0).wait_send()
            z_copy(j).wait_send()
            for d in span:
                w_hub(j, 0, d, grp).wait_send()
                w_hub(j, 1, d, grp).wait_send()
                if keep:
                    w_keep(j, d).wait_send()

        @pl.when(leaf)
        def _():
            w_pair(j, 1).wait_send()

    loop(0, pieces, drain)
    for s in range(slots):
        for g in range(groups):
            for k in range(2):
                x_y(s, g, k).wait_send()

    @pl.when(leaf)
    def _():
        for p in range(2 * slots):
            for d in span:
                for k in range(2):
                    x_z(p, d, k).wait_send()

    for h in range(heads):
        out_copy(h).wait()


def body(tokens, queries, gains, key_weight, value_weight, lengths):
    n = lax.axis_size(AXIS)
    _, slots, tok, depth = tokens.shape
    _, rows, key_width = key_weight.shape
    heads = key_width // HEAD
    pieces = 2 * heads
    groups = n // 4
    total = slots * tok
    keep = rows // 2 // HEAD * HEAD
    bf, f32 = jnp.bfloat16, jnp.float32
    any_spec = pl.BlockSpec(memory_space=pl.ANY)
    vmem_spec = pl.BlockSpec(memory_space=pltpu.VMEM)
    dma = pltpu.SemaphoreType.DMA
    fan = groups - 1
    return pl.pallas_call(
        functools.partial(kernel, n, keep),
        out_shape=jax.ShapeDtypeStruct(queries.shape, bf),
        in_specs=[any_spec, any_spec, vmem_spec, any_spec, any_spec, vmem_spec],
        out_specs=any_spec,
        scratch_shapes=[
            pltpu.VMEM((slots, tok, depth), bf),
            pltpu.VMEM(queries.shape[1:], bf),
            pltpu.VMEM(queries.shape[1:], bf),
            pltpu.VMEM((pieces, groups, 2, rows, HEAD), bf),
            pltpu.VMEM((groups, 2, 2 * total, rows), bf),
            pltpu.VMEM((groups, 2, total, rows), bf),
            pltpu.VMEM((groups, 2, 2 * total, rows), bf),
            pltpu.VMEM((pieces, 2 * total, HEAD), f32),
            pltpu.VMEM((pieces, 2 * total, HEAD), bf),
            pltpu.VMEM((pieces, 2 * total, HEAD), bf),
            pltpu.VMEM((pieces, total, HEAD), bf),
            pltpu.VMEM((pieces, total, HEAD), bf),
            pltpu.VMEM((pieces, total, HEAD), bf),
            pltpu.VMEM((pieces, total, HEAD), bf),
            pltpu.VMEM((slots, tok, HEAD), jnp.int32),
            dma((pieces,)), dma((slots,)), dma, dma((heads,)),
            dma((pieces,)), dma((pieces,)),
            dma((pieces, 2, fan)), dma((pieces, 2, groups)),
            dma((pieces, fan)), dma((pieces, fan)),
            dma((slots, groups, 2)), dma((slots, groups, 2)),
            dma((2 * slots, fan, 2)), dma((2 * slots, fan, 2)),
            dma((pieces,)), dma((pieces,)),
            dma((pieces,)), dma((pieces,)),
            dma((pieces,)), dma((pieces,)),
        ],
        compiler_params=pltpu.CompilerParams(
            collective_id=0, has_side_effects=True, vmem_limit_bytes=60 * 1024 * 1024
        ),
    )(tokens, queries, gains, key_weight, value_weight, lengths)


def solution(mesh):
    return jax.shard_map(
        body,
        mesh=mesh,
        in_specs=(
            P("section", None, "fsdp", None),
            P("section", None, "fsdp", None),
            P("section", None),
            P("section", "fsdp", None),
            P("section", "fsdp", None),
            P(),
        ),
        out_specs=P("section", None, "fsdp", None),
        check_vma=False,
    )
```

```python
import functools

import jax
import jax.numpy as jnp
from jax import lax
from jax.experimental import pallas as pl
from jax.experimental.pallas import tpu as pltpu
from jax.sharding import PartitionSpec as P

HEAD = 128
AXIS = "fsdp"
LEAD = 2
LAG = 2
EARLY = 2


def kernel(
    n, keep,
    x_hbm, q_hbm, gain_ref, kw_hbm, vw_hbm, len_ref, o_hbm,
    x_v, q_v, o_v, wbuf, xs, sx, lx, acc, ls, lr, zs, zr, ys, yr, es, er, kv, kx, prior, side, weights, start_s,
    lw_sem, lx_sem, lq_sem, lo_sem,
    wz_s, wz_r, wh_s, wh_r, wk_s, wk_r, xy_s, xy_r, xz_s, xz_r,
    l_s, l_r, z_s, z_r, y_s, y_r, e_s, e_r, p_s, p_r, r_s,
):
    slots, tok, depth = x_v.shape
    pieces, groups, _, rows, _ = wbuf.shape
    heads = pieces // 2
    total = slots * tok
    q_per_kv = q_v.shape[2] // (heads * HEAD)
    me = lax.axis_index(AXIS)
    bit = me % 2
    cls = (me // 2) % 2
    grp = me // 4
    leaf = cls == grp % 2
    hub = jnp.logical_not(leaf)
    kind = jnp.where(leaf, 1, 0)
    y_peer = me + 1 - 2 * bit
    z_peer = me + 2 - 4 * cls
    right = lax.rem(me + 1, n)
    left = lax.rem(me + n - 1, n)
    others = [lax.rem(grp + d, groups) for d in range(1, groups)]
    span = range(len(others))
    cross = (me % 4 == 3) & (grp % 2 == 0) & (me < n - 1)
    relay = (me % 4 == 2) & (grp % 2 == 0) & (me < n - 2)
    far = (me % 4 == 0) & (grp % 2 == 1)

    def hub_of(g):
        return 4 * g + 2 * (1 - g % 2) + bit

    def load_w(j):
        w = vw_hbm if j % 2 else kw_hbm
        cols = pl.ds((j // 2) * HEAD, HEAD)
        return pltpu.make_async_copy(w.at[0, :, cols], wbuf.at[j, grp, kind], lw_sem.at[j])

    x_loads = [pltpu.make_async_copy(x_hbm.at[0, s], x_v.at[s], lx_sem.at[s]) for s in range(slots)]
    q_load = pltpu.make_async_copy(q_hbm.at[0], q_v, lq_sem)
    w_loads = [load_w(j) for j in range(pieces)]
    for copy in w_loads[:2] + x_loads[:1] + w_loads[2:] + x_loads[1:] + [q_load]:
        copy.start()

    barrier = pltpu.get_barrier_semaphore()

    def greet(peer):
        pl.semaphore_signal(barrier, inc=1, device_id={AXIS: peer}, device_id_type=pl.DeviceIdType.MESH)

    greet(y_peer)
    greet(z_peer)

    @pl.when(hub)
    def _():
        for g in others:
            greet(hub_of(g))

    @pl.when(me < n - 1)
    def _():
        greet(right)

    @pl.when(relay)
    def _():
        greet(lax.rem(me + 2, n))

    @pl.when(far)
    def _():
        greet(me - 2)

    @pl.when(me > 0)
    def _():
        greet(left)

    prior[...] = jnp.zeros_like(prior)
    pl.semaphore_wait(
        barrier,
        2 + jnp.where(hub, len(others), 0) + jnp.where(me < n - 1, 1, 0) + jnp.where(me > 0, 1, 0)
        + jnp.where(relay, 1, 0) + jnp.where(far, 1, 0),
    )

    def remote(src, dst, send, recv, peer):
        return pltpu.make_async_remote_copy(
            src_ref=src, dst_ref=dst, send_sem=send, recv_sem=recv,
            device_id={AXIS: peer}, device_id_type=pl.DeviceIdType.MESH,
        )

    def w_pair(j, k):
        block = wbuf.at[j, grp, k]
        return remote(block, block, wz_s.at[j], wz_r.at[j], z_peer)

    def w_hub(j, k, d, g):
        block = wbuf.at[j, g, k]
        return remote(block, block, wh_s.at[j, k, d], wh_r.at[j, k, g], hub_of(others[d]))

    def w_keep(j, d):
        block = wbuf.at[j, others[d], 0, pl.ds(0, keep)]
        return remote(block, block, wk_s.at[j, d], wk_r.at[j, d], z_peer)

    def x_y(s, g, k):
        return remote(
            sx.at[g, k, pl.ds(s * tok, tok)], xs.at[g, k, pl.ds(total + s * tok, tok)],
            xy_s.at[s, g, k], xy_r.at[s, g, k], y_peer,
        )

    def x_z(p, d, k):
        skip = 0 if k else keep
        here = (others[d], k, pl.ds(p * tok, tok), pl.ds(skip, rows - skip))
        return remote(xs.at[here], lx.at[here], xz_s.at[p, d, k], xz_r.at[p, d, k], z_peer)

    def l_copy(j):
        return remote(ls.at[j], lr.at[j], l_s.at[j], l_r.at[j], y_peer)

    def z_copy(j):
        return remote(zs.at[j], zr.at[j], z_s.at[j], z_r.at[j], z_peer)

    def y_copy(j):
        return remote(ys.at[j], yr.at[j], y_s.at[j], y_r.at[j], y_peer)

    def e_copy(j):
        return remote(es.at[j], er.at[j], e_s.at[j], e_r.at[j], y_peer)

    def p_copy(j):
        return remote(kv.at[j], prior.at[j], p_s.at[j], p_r.at[j], right)

    def r_copy(j):
        return remote(kx.at[j], prior.at[j], r_s.at[j], p_r.at[j], lax.rem(me + 2, n))

    for j in range(pieces):
        w_loads[j].wait()

        @pl.when(hub)
        def _(j=j):
            w_pair(j, 0).start()
            for d in span:
                w_hub(j, 0, d, grp).start()

        if j < LEAD:
            @pl.when(leaf)
            def _(j=j):
                w_pair(j, 1).start()

    block_rows = 16

    def norm_block(s, r):
        here = pl.ds(pl.multiple_of(r * block_rows, block_rows), block_rows)
        there = pl.ds(pl.multiple_of(s * tok + r * block_rows, block_rows), block_rows)
        squares = jnp.zeros((block_rows, 1), jnp.float32)
        step = 4 * HEAD
        for i in range(depth // step):
            piece = x_v[s, here, i * step:(i + 1) * step].astype(jnp.float32)
            squares = squares + jnp.sum(piece * piece, axis=-1, keepdims=True)
        inverse = lax.rsqrt(squares / depth + 1e-05)
        for g in range(groups):
            for k in range(2):
                line = g % 2 if k else 1 - g % 2
                for mine in (False, True):
                    first = (4 * g + 2 * line + (bit if mine else 1 - bit)) * rows
                    cols = pl.ds(pl.multiple_of(first, HEAD), rows)
                    value = x_v[s, here, cols].astype(jnp.float32) * inverse
                    value = (value * gain_ref[0:1, cols].astype(jnp.float32)).astype(jnp.bfloat16)
                    if mine:
                        xs[g, k, there, :] = value
                    else:
                        sx[g, k, there, :] = value

    for s in range(slots):
        x_loads[s].wait()

        def norm_step(r, carry, s=s):
            norm_block(s, r)
            return carry

        lax.fori_loop(0, tok // block_rows, norm_step, 0)
        for g in others + [grp]:
            for k in range(2):
                x_y(s, g, k).start()

        @pl.when(leaf)
        def _(s=s):
            for d in span:
                for k in range(2):
                    x_z(s, d, k).start()

    docs = len_ref.shape[1]
    rowi = lax.broadcasted_iota(jnp.int32, (docs, docs), 0)
    coli = lax.broadcasted_iota(jnp.int32, (docs, docs), 1)
    pos = lax.broadcasted_iota(jnp.int32, (tok, 1), 0) + me * tok
    for s in range(slots):
        lens = jnp.broadcast_to(len_ref[s:s + 1, :], (docs, docs))
        bounds = jnp.sum(jnp.where(coli <= rowi, lens, 0), axis=1, keepdims=True)
        bound_row = jnp.sum(jnp.where(coli == rowi, bounds, 0), axis=0, keepdims=True)
        start = jnp.max(jnp.where(bound_row <= pos, bound_row, 0), axis=1, keepdims=True)
        start_s[s] = jnp.broadcast_to(start, (tok, HEAD))
    q_load.wait()

    def dot(a, b):
        return jnp.dot(a, b, preferred_element_type=jnp.float32)

    def loop(lo, hi, step):
        def run(j, carry):
            step(j)
            return carry

        lax.fori_loop(lo, hi, run, 0)

    def take_hub(j):
        for d in span:
            w_hub(j, 0, d, others[d]).wait_recv()
            if keep:
                w_keep(j, d).start()

    def pass_leaf(j):
        w_pair(j, 1).wait_recv()
        for d in span:
            w_hub(j, 1, d, grp).start()

    @pl.when(hub)
    def _():
        loop(0, pieces // 2, take_hub)
        loop(0, LEAD, pass_leaf)
        loop(pieces // 2, pieces, take_hub)
        for s in range(slots):
            for g in others + [grp]:
                for k in range(2):
                    x_y(s, g, k).wait_recv()

        def first(j):
            value = dot(xs[grp, 0], wbuf[j, grp, 0])
            for g in others:
                value = value + dot(xs[g, 0], wbuf[j, g, 0])
            acc[j] = value

        loop(0, pieces, first)
        for p in range(2 * slots):
            for d in span:
                for k in range(2):
                    x_z(p, d, k).wait_recv()

    @pl.when(leaf)
    def _():
        for s in range(slots):
            for d in span:
                for k in range(2):
                    x_y(s, others[d], k).wait_recv()
                    x_z(slots + s, d, k).start()

        def send_w(j):
            w_pair(j, 1).start()

        loop(LEAD, pieces, send_w)
        for s in range(slots):
            for k in range(2):
                x_y(s, grp, k).wait_recv()

        def first(j):
            w_pair(j, 0).wait_recv()
            acc[j] = dot(xs[grp, 0], wbuf[j, grp, 0]) + dot(xs[grp, 1], wbuf[j, grp, 1])

        loop(0, pieces, first)
        def second(j):
            value = acc[j]
            if keep:
                for d in span:
                    w_keep(j, d).wait_recv()
                    value = value + dot(
                        xs[others[d], 0, :, 0:keep], wbuf[j, others[d], 0, 0:keep]
                    )
                acc[j] = value
            ys[j] = value[total:].astype(jnp.bfloat16)
            y_copy(j).start()

        loop(0, pieces, second)

    def send_prior(j):
        @pl.when(me < n - 1)
        def _():
            p_copy(j).start()

    def cross_over(j):
        @pl.when(cross & (j % 2 == 1))
        def _():
            p_copy(j).start()

        @pl.when(relay & (j % 2 == 0))
        def _():
            r_copy(j).start()

    def meet_hub(j):
        for d in span:
            w_hub(j, 1, d, others[d]).wait_recv()
        part = jnp.zeros((2 * total, HEAD), jnp.float32)
        for g in others:
            part = part + dot(lx[g, 0, :, keep:], wbuf[j, g, 0, keep:])
            part = part + dot(lx[g, 1], wbuf[j, g, 1])
        ls[j] = part[total:].astype(jnp.bfloat16)
        l_copy(j).start()
        value = acc[j] + dot(xs[grp, 1], wbuf[j, grp, 1])
        for g in others:
            value = value + dot(xs[g, 1], wbuf[j, g, 1])
        ys[j] = value[total:].astype(jnp.bfloat16)
        y_copy(j).start()
        acc[j, 0:total] = value[:total]
        acc[j, total:] = part[:total]

        @pl.when(cross & (j % 2 == 0))
        def _():
            es[j] = value[:total].astype(jnp.bfloat16)
            e_copy(j).start()

        @pl.when(relay & (j % 2 == 0))
        def _():
            side[j] = value[total:]

    def settle_hub(j):
        l_copy(j).wait_recv()
        zs[j] = (acc[j, total:] + lr[j].astype(jnp.float32)).astype(jnp.bfloat16)
        z_copy(j).start()
        y_copy(j).wait_recv()
        kv[j] = (acc[j, 0:total] + yr[j].astype(jnp.float32)).astype(jnp.bfloat16)

        @pl.when(jnp.logical_not(cross))
        def _():
            send_prior(j)

        @pl.when(relay & (j % 2 == 0))
        def _():
            e_copy(j).wait_recv()
            kx[j] = (side[j] + er[j].astype(jnp.float32)).astype(jnp.bfloat16)

        held = pieces - LEAD - 2

        @pl.when((j < EARLY) | (j > held))
        def _():
            cross_over(j)

        @pl.when(j == held)
        def _():
            loop(EARLY, held + 1, cross_over)

    def meet_leaf(j):
        y_copy(j).wait_recv()
        z_copy(j).wait_recv()
        kv[j] = (
            acc[j, 0:total] + yr[j].astype(jnp.float32) + zr[j].astype(jnp.float32)
        ).astype(jnp.bfloat16)
        send_prior(j)

    lane = lax.broadcasted_iota(jnp.int32, (tok, tok), 1)
    own = lane <= lax.broadcasted_iota(jnp.int32, (tok, tok), 0)
    key_pos = lane + jnp.where(own, me, me - 1) * tok
    wide = q_per_kv * HEAD

    def out_copy(h):
        cols = pl.ds(pl.multiple_of(h * wide, HEAD), wide)
        return pltpu.make_async_copy(o_v.at[:, :, cols], o_hbm.at[0, :, :, cols], lo_sem.at[h])

    def wait_prior(j):
        @pl.when(me > 0)
        def _():
            p_copy(j).wait_recv()

    def weigh(h):
        wait_prior(2 * h)
        for s in range(slots):
            here = slice(s * tok, (s + 1) * tok)
            keys = jnp.concatenate([prior[2 * h, here], kv[2 * h, here]], axis=0)
            allowed = key_pos >= start_s[s]
            for q in range(q_per_kv):
                cols = pl.ds(pl.multiple_of((h * q_per_kv + q) * HEAD, HEAD), HEAD)
                both = lax.dot_general(
                    q_v[s, :, cols], keys, (((1,), (1,)), ((), ())),
                    preferred_element_type=jnp.float32,
                )
                scores = jnp.where(own, both[:, tok:], both[:, :tok]) * HEAD ** (-0.5)
                scores = jnp.where(allowed, scores, -1e30)
                maxima = jnp.max(scores, axis=-1, keepdims=True)
                exponent = jnp.exp(scores - maxima)
                sums = jnp.sum(exponent, axis=-1, keepdims=True)
                soft = exponent * (1.0 / sums)
                weights[s, q, :, 0:tok] = jnp.where(own, 0.0, soft).astype(jnp.bfloat16)
                weights[s, q, :, tok:] = jnp.where(own, soft, 0.0).astype(jnp.bfloat16)

    def mix(h):
        wait_prior(2 * h + 1)
        for s in range(slots):
            here = slice(s * tok, (s + 1) * tok)
            values = jnp.concatenate([prior[2 * h + 1, here], kv[2 * h + 1, here]], axis=0)
            for q in range(q_per_kv):
                cols = pl.ds(pl.multiple_of((h * q_per_kv + q) * HEAD, HEAD), HEAD)
                o_v[s, :, cols] = dot(weights[s, q], values).astype(jnp.bfloat16)
        out_copy(h).start()

    @pl.when(hub)
    def _():
        first_late = jnp.where(far, EARLY // 2, heads - LAG)

        def step(j):
            meet_hub(j)

            @pl.when(j + LEAD < pieces)
            def _():
                pass_leaf(j + LEAD)

            @pl.when(j > 0)
            def _():
                settle_hub(j - 1)

            @pl.when((j % 2 == 1) & (j > 2 * LAG) & (j // 2 - LAG < first_late))
            def _():
                weigh(j // 2 - LAG)
                mix(j // 2 - LAG)

        loop(0, pieces, step)
        settle_hub(pieces - 1)

        def rest(h):
            weigh(h)
            mix(h)

        loop(first_late, heads, rest)

    @pl.when(leaf)
    def _():
        def step(h):
            meet_leaf(2 * h)

            @pl.when(h > 0)
            def _():
                mix(h - 1)

            weigh(h)
            meet_leaf(2 * h + 1)

        loop(0, heads, step)
        mix(heads - 1)

    def drain(j):
        y_copy(j).wait_send()

        @pl.when((me < n - 1) & jnp.logical_not(cross & (j % 2 == 0)))
        def _():
            p_copy(j).wait_send()

        @pl.when(cross & (j % 2 == 0))
        def _():
            e_copy(j).wait_send()

        @pl.when(relay & (j % 2 == 0))
        def _():
            r_copy(j).wait_send()

        @pl.when(hub)
        def _():
            w_pair(j, 0).wait_send()
            l_copy(j).wait_send()
            z_copy(j).wait_send()
            for d in span:
                w_hub(j, 0, d, grp).wait_send()
                w_hub(j, 1, d, grp).wait_send()
                if keep:
                    w_keep(j, d).wait_send()

        @pl.when(leaf)
        def _():
            w_pair(j, 1).wait_send()

    loop(0, pieces, drain)
    for s in range(slots):
        for g in range(groups):
            for k in range(2):
                x_y(s, g, k).wait_send()

    @pl.when(leaf)
    def _():
        for p in range(2 * slots):
            for d in span:
                for k in range(2):
                    x_z(p, d, k).wait_send()

    for h in range(heads):
        out_copy(h).wait()


def body(tokens, queries, gains, key_weight, value_weight, lengths):
    n = lax.axis_size(AXIS)
    _, slots, tok, depth = tokens.shape
    _, rows, key_width = key_weight.shape
    heads = key_width // HEAD
    pieces = 2 * heads
    groups = n // 4
    total = slots * tok
    keep = rows // 2 // HEAD * HEAD
    bf, f32 = jnp.bfloat16, jnp.float32
    any_spec = pl.BlockSpec(memory_space=pl.ANY)
    vmem_spec = pl.BlockSpec(memory_space=pltpu.VMEM)
    dma = pltpu.SemaphoreType.DMA
    fan = groups - 1
    return pl.pallas_call(
        functools.partial(kernel, n, keep),
        out_shape=jax.ShapeDtypeStruct(queries.shape, bf),
        in_specs=[any_spec, any_spec, vmem_spec, any_spec, any_spec, vmem_spec],
        out_specs=any_spec,
        scratch_shapes=[
            pltpu.VMEM((slots, tok, depth), bf),
            pltpu.VMEM(queries.shape[1:], bf),
            pltpu.VMEM(queries.shape[1:], bf),
            pltpu.VMEM((pieces, groups, 2, rows, HEAD), bf),
            pltpu.VMEM((groups, 2, 2 * total, rows), bf),
            pltpu.VMEM((groups, 2, total, rows), bf),
            pltpu.VMEM((groups, 2, 2 * total, rows), bf),
            pltpu.VMEM((pieces, 2 * total, HEAD), f32),
            pltpu.VMEM((pieces, total, HEAD), bf),
            pltpu.VMEM((pieces, total, HEAD), bf),
            pltpu.VMEM((pieces, total, HEAD), bf),
            pltpu.VMEM((pieces, total, HEAD), bf),
            pltpu.VMEM((pieces, total, HEAD), bf),
            pltpu.VMEM((pieces, total, HEAD), bf),
            pltpu.VMEM((pieces, total, HEAD), bf),
            pltpu.VMEM((pieces, total, HEAD), bf),
            pltpu.VMEM((pieces, total, HEAD), bf),
            pltpu.VMEM((pieces, total, HEAD), bf),
            pltpu.VMEM((pieces, total, HEAD), bf),
            pltpu.VMEM((pieces, total, HEAD), f32),
            pltpu.VMEM((slots, queries.shape[-1] // key_width, tok, 2 * tok), bf),
            pltpu.VMEM((slots, tok, HEAD), jnp.int32),
            dma((pieces,)), dma((slots,)), dma, dma((heads,)),
            dma((pieces,)), dma((pieces,)),
            dma((pieces, 2, fan)), dma((pieces, 2, groups)),
            dma((pieces, fan)), dma((pieces, fan)),
            dma((slots, groups, 2)), dma((slots, groups, 2)),
            dma((2 * slots, fan, 2)), dma((2 * slots, fan, 2)),
            dma((pieces,)), dma((pieces,)),
            dma((pieces,)), dma((pieces,)),
            dma((pieces,)), dma((pieces,)),
            dma((pieces,)), dma((pieces,)),
            dma((pieces,)), dma((pieces,)), dma((pieces,)),
        ],
        compiler_params=pltpu.CompilerParams(
            collective_id=0, has_side_effects=True, vmem_limit_bytes=60 * 1024 * 1024
        ),
    )(tokens, queries, gains, key_weight, value_weight, lengths)


def solution(mesh):
    return jax.shard_map(
        body,
        mesh=mesh,
        in_specs=(
            P("section", None, "fsdp", None),
            P("section", None, "fsdp", None),
            P("section", None),
            P("section", "fsdp", None),
            P("section", "fsdp", None),
            P(),
        ),
        out_specs=P("section", None, "fsdp", None),
        check_vma=False,
    )
```

```python
import functools

import jax
import jax.numpy as jnp
from jax import lax
from jax.experimental import pallas as pl
from jax.experimental.pallas import tpu as pltpu
from jax.sharding import PartitionSpec as P

HEAD = 128
AXIS = "fsdp"
LEAD = 2
LAG = 2
EARLY = 2


def kernel(
    n, keep,
    x_hbm, q_hbm, gain_ref, kw_hbm, vw_hbm, len_ref, o_hbm,
    x_v, q_v, o_v, wbuf, xs, sx, lx, acc, ls, lr, zs, zr, ys, yr, es, er, fs, fr, kv, kx, kq, prior, side, behind, part_s, weights, start_s,
    lw_sem, lx_sem, lq_sem, lo_sem,
    wz_s, wz_r, wh_s, wh_r, wk_s, wk_r, xy_s, xy_r, xz_s, xz_r,
    l_s, l_r, z_s, z_r, y_s, y_r, e_s, e_r, f_s, f_r, p_s, p_r, q_s, q_r, r_s,
):
    slots, tok, depth = x_v.shape
    pieces, groups, _, rows, _ = wbuf.shape
    heads = pieces // 2
    total = slots * tok
    q_per_kv = q_v.shape[2] // (heads * HEAD)
    me = lax.axis_index(AXIS)
    bit = me % 2
    cls = (me // 2) % 2
    grp = me // 4
    leaf = cls == grp % 2
    hub = jnp.logical_not(leaf)
    kind = jnp.where(leaf, 1, 0)
    y_peer = me + 1 - 2 * bit
    z_peer = me + 2 - 4 * cls
    right = lax.rem(me + 1, n)
    left = lax.rem(me + n - 1, n)
    others = [lax.rem(grp + d, groups) for d in range(1, groups)]
    span = range(len(others))
    cross = (me % 4 == 3) & (grp % 2 == 0) & (me < n - 1)
    relay = (me % 4 == 2) & (grp % 2 == 0) & (me < n - 2)
    far = (me % 4 == 0) & (grp % 2 == 1)
    base = (me % 4 == 0) & (grp % 2 == 0)
    rear = (me % 4 == 1) & (grp % 2 == 0)
    front = (me % 4 == 2) & (grp % 2 == 0)
    mate = (me % 4 == 3) & (grp % 2 == 0)

    def hub_of(g):
        return 4 * g + 2 * (1 - g % 2) + bit

    def load_w(j):
        w = vw_hbm if j % 2 else kw_hbm
        cols = pl.ds((j // 2) * HEAD, HEAD)
        return pltpu.make_async_copy(w.at[0, :, cols], wbuf.at[j, grp, kind], lw_sem.at[j])

    x_loads = [pltpu.make_async_copy(x_hbm.at[0, s], x_v.at[s], lx_sem.at[s]) for s in range(slots)]
    q_load = pltpu.make_async_copy(q_hbm.at[0], q_v, lq_sem)
    w_loads = [load_w(j) for j in range(pieces)]
    for copy in w_loads[:2] + x_loads[:1] + w_loads[2:] + x_loads[1:] + [q_load]:
        copy.start()

    barrier = pltpu.get_barrier_semaphore()

    def greet(peer):
        pl.semaphore_signal(barrier, inc=1, device_id={AXIS: peer}, device_id_type=pl.DeviceIdType.MESH)

    greet(y_peer)
    greet(z_peer)

    @pl.when(hub)
    def _():
        for g in others:
            greet(hub_of(g))

    @pl.when(me < n - 1)
    def _():
        greet(right)

    @pl.when(relay)
    def _():
        greet(lax.rem(me + 2, n))

    @pl.when(far)
    def _():
        greet(me - 2)

    @pl.when(me > 0)
    def _():
        greet(left)

    prior[...] = jnp.zeros_like(prior)
    pl.semaphore_wait(
        barrier,
        2 + jnp.where(hub, len(others), 0) + jnp.where(me < n - 1, 1, 0) + jnp.where(me > 0, 1, 0)
        + jnp.where(relay, 1, 0) + jnp.where(far, 1, 0),
    )

    def remote(src, dst, send, recv, peer):
        return pltpu.make_async_remote_copy(
            src_ref=src, dst_ref=dst, send_sem=send, recv_sem=recv,
            device_id={AXIS: peer}, device_id_type=pl.DeviceIdType.MESH,
        )

    def w_pair(j, k):
        block = wbuf.at[j, grp, k]
        return remote(block, block, wz_s.at[j], wz_r.at[j], z_peer)

    def w_hub(j, k, d, g):
        block = wbuf.at[j, g, k]
        return remote(block, block, wh_s.at[j, k, d], wh_r.at[j, k, g], hub_of(others[d]))

    def w_keep(j, d):
        block = wbuf.at[j, others[d], 0, pl.ds(0, keep)]
        return remote(block, block, wk_s.at[j, d], wk_r.at[j, d], z_peer)

    def x_y(s, g, k):
        return remote(
            sx.at[g, k, pl.ds(s * tok, tok)], xs.at[g, k, pl.ds(total + s * tok, tok)],
            xy_s.at[s, g, k], xy_r.at[s, g, k], y_peer,
        )

    def x_z(p, d, k):
        skip = 0 if k else keep
        here = (others[d], k, pl.ds(p * tok, tok), pl.ds(skip, rows - skip))
        return remote(xs.at[here], lx.at[here], xz_s.at[p, d, k], xz_r.at[p, d, k], z_peer)

    def l_copy(j):
        return remote(ls.at[j], lr.at[j], l_s.at[j], l_r.at[j], y_peer)

    def z_copy(j):
        return remote(zs.at[j], zr.at[j], z_s.at[j], z_r.at[j], z_peer)

    def y_copy(j):
        return remote(ys.at[j], yr.at[j], y_s.at[j], y_r.at[j], y_peer)

    def e_copy(j):
        return remote(es.at[j], er.at[j], e_s.at[j], e_r.at[j], y_peer)

    def f_copy(j):
        return remote(fs.at[j], fr.at[j], f_s.at[j], f_r.at[j], y_peer)

    def q_copy(j):
        return remote(kx.at[j], kq.at[j], q_s.at[j], q_r.at[j], z_peer)

    def p_copy(j):
        return remote(kv.at[j], prior.at[j], p_s.at[j], p_r.at[j], right)

    def r_copy(j):
        return remote(kx.at[j], prior.at[j], r_s.at[j], p_r.at[j], lax.rem(me + 2, n))

    for j in range(pieces):
        w_loads[j].wait()

        @pl.when(hub)
        def _(j=j):
            w_pair(j, 0).start()
            for d in span:
                w_hub(j, 0, d, grp).start()

        if j < LEAD:
            @pl.when(leaf)
            def _(j=j):
                w_pair(j, 1).start()

    block_rows = 16

    def norm_block(s, r):
        here = pl.ds(pl.multiple_of(r * block_rows, block_rows), block_rows)
        there = pl.ds(pl.multiple_of(s * tok + r * block_rows, block_rows), block_rows)
        squares = jnp.zeros((block_rows, 1), jnp.float32)
        step = 4 * HEAD
        for i in range(depth // step):
            piece = x_v[s, here, i * step:(i + 1) * step].astype(jnp.float32)
            squares = squares + jnp.sum(piece * piece, axis=-1, keepdims=True)
        inverse = lax.rsqrt(squares / depth + 1e-05)
        for g in range(groups):
            for k in range(2):
                line = g % 2 if k else 1 - g % 2
                for mine in (False, True):
                    first = (4 * g + 2 * line + (bit if mine else 1 - bit)) * rows
                    cols = pl.ds(pl.multiple_of(first, HEAD), rows)
                    value = x_v[s, here, cols].astype(jnp.float32) * inverse
                    value = (value * gain_ref[0:1, cols].astype(jnp.float32)).astype(jnp.bfloat16)
                    if mine:
                        xs[g, k, there, :] = value
                    else:
                        sx[g, k, there, :] = value

    for s in range(slots):
        x_loads[s].wait()

        def norm_step(r, carry, s=s):
            norm_block(s, r)
            return carry

        lax.fori_loop(0, tok // block_rows, norm_step, 0)
        for g in others + [grp]:
            for k in range(2):
                x_y(s, g, k).start()

        @pl.when(leaf)
        def _(s=s):
            for d in span:
                for k in range(2):
                    x_z(s, d, k).start()

    docs = len_ref.shape[1]
    rowi = lax.broadcasted_iota(jnp.int32, (docs, docs), 0)
    coli = lax.broadcasted_iota(jnp.int32, (docs, docs), 1)
    pos = lax.broadcasted_iota(jnp.int32, (tok, 1), 0) + me * tok
    for s in range(slots):
        lens = jnp.broadcast_to(len_ref[s:s + 1, :], (docs, docs))
        bounds = jnp.sum(jnp.where(coli <= rowi, lens, 0), axis=1, keepdims=True)
        bound_row = jnp.sum(jnp.where(coli == rowi, bounds, 0), axis=0, keepdims=True)
        start = jnp.max(jnp.where(bound_row <= pos, bound_row, 0), axis=1, keepdims=True)
        start_s[s] = jnp.broadcast_to(start, (tok, HEAD))
    q_load.wait()

    def dot(a, b):
        return jnp.dot(a, b, preferred_element_type=jnp.float32)

    def loop(lo, hi, step):
        def run(j, carry):
            step(j)
            return carry

        lax.fori_loop(lo, hi, run, 0)

    def take_hub(j):
        for d in span:
            w_hub(j, 0, d, others[d]).wait_recv()
            if keep:
                w_keep(j, d).start()

    def pass_leaf(j):
        w_pair(j, 1).wait_recv()
        for d in span:
            w_hub(j, 1, d, grp).start()

    @pl.when(hub)
    def _():
        loop(0, pieces // 2, take_hub)
        loop(0, LEAD, pass_leaf)
        loop(pieces // 2, pieces, take_hub)
        for s in range(slots):
            for g in others + [grp]:
                for k in range(2):
                    x_y(s, g, k).wait_recv()

        def first(j):
            value = dot(xs[grp, 0], wbuf[j, grp, 0])
            for g in others:
                value = value + dot(xs[g, 0], wbuf[j, g, 0])
            acc[j] = value

        loop(0, pieces, first)
        for p in range(2 * slots):
            for d in span:
                for k in range(2):
                    x_z(p, d, k).wait_recv()

    @pl.when(leaf)
    def _():
        for s in range(slots):
            for d in span:
                for k in range(2):
                    x_y(s, others[d], k).wait_recv()
                    x_z(slots + s, d, k).start()

        def send_w(j):
            w_pair(j, 1).start()

        loop(LEAD, pieces, send_w)
        for s in range(slots):
            for k in range(2):
                x_y(s, grp, k).wait_recv()

        def first(j):
            w_pair(j, 0).wait_recv()
            acc[j] = dot(xs[grp, 0], wbuf[j, grp, 0]) + dot(xs[grp, 1], wbuf[j, grp, 1])

        loop(0, pieces, first)
        def second(j):
            value = acc[j]
            if keep:
                for d in span:
                    w_keep(j, d).wait_recv()
                    value = value + dot(
                        xs[others[d], 0, :, 0:keep], wbuf[j, others[d], 0, 0:keep]
                    )
                acc[j] = value
            ys[j] = value[total:].astype(jnp.bfloat16)
            y_copy(j).start()

            @pl.when(rear)
            def _():
                es[j] = value[:total].astype(jnp.bfloat16)
                e_copy(j).start()

        loop(0, pieces, second)

    def send_prior(j):
        @pl.when((me < n - 1) & jnp.logical_not(cross) & jnp.logical_not(rear))
        def _():
            p_copy(j).start()

    def cross_over(j):
        @pl.when(cross & (j % 2 == 1))
        def _():
            p_copy(j).start()

        @pl.when(relay & (j % 2 == 0))
        def _():
            r_copy(j).start()

    held = pieces - LEAD - 2

    def meet_hub(j):
        part = jnp.zeros((2 * total, HEAD), jnp.float32)
        for g in others:
            part = part + dot(lx[g, 0, :, keep:], wbuf[j, g, 0, keep:])
        part_s[...] = part
        acc[j] = acc[j] + dot(xs[grp, 1], wbuf[j, grp, 1])
        for d in span:
            w_hub(j, 1, d, others[d]).wait_recv()
        part = part_s[...]
        for g in others:
            part = part + dot(lx[g, 1], wbuf[j, g, 1])
        ls[j] = part[total:].astype(jnp.bfloat16)
        l_copy(j).start()
        value = acc[j]
        for g in others:
            value = value + dot(xs[g, 1], wbuf[j, g, 1])
        ys[j] = value[total:].astype(jnp.bfloat16)
        y_copy(j).start()
        acc[j, 0:total] = value[:total]
        acc[j, total:] = part[:total]

        @pl.when(mate)
        def _():
            fs[j] = part[:total].astype(jnp.bfloat16)
            f_copy(j).start()

        @pl.when(cross & (j % 2 == 0))
        def _():
            es[j] = value[:total].astype(jnp.bfloat16)
            e_copy(j).start()

        @pl.when(front)
        def _():
            behind[j] = part[total:]

        @pl.when(relay & (j % 2 == 0))
        def _():
            side[j] = value[total:]

    def settle_hub(j):
        l_copy(j).wait_recv()
        zs[j] = (acc[j, total:] + lr[j].astype(jnp.float32)).astype(jnp.bfloat16)
        z_copy(j).start()
        y_copy(j).wait_recv()
        kv[j] = (acc[j, 0:total] + yr[j].astype(jnp.float32)).astype(jnp.bfloat16)
        send_prior(j)

        @pl.when(relay & (j % 2 == 0))
        def _():
            e_copy(j).wait_recv()
            kx[j] = (side[j] + er[j].astype(jnp.float32)).astype(jnp.bfloat16)

        @pl.when((j < EARLY) | (j > held))
        def _():
            cross_over(j)

        @pl.when(j == held)
        def _():
            loop(EARLY, held + 1, cross_over)

    def gather_leaf(j):
        y_copy(j).wait_recv()
        value = acc[j, 0:total] + yr[j].astype(jnp.float32)
        acc[j, 0:total] = value

        @pl.when(base)
        def _():
            e_copy(j).wait_recv()
            kx[j] = (acc[j, total:] + er[j].astype(jnp.float32)).astype(jnp.bfloat16)
            q_copy(j).start()

    def meet_leaf(j):
        z_copy(j).wait_recv()
        kv[j] = (acc[j, 0:total] + zr[j].astype(jnp.float32)).astype(jnp.bfloat16)
        send_prior(j)

    lane = lax.broadcasted_iota(jnp.int32, (tok, tok), 1)
    own = lane <= lax.broadcasted_iota(jnp.int32, (tok, tok), 0)
    key_pos = lane + jnp.where(own, me, me - 1) * tok
    wide = q_per_kv * HEAD

    def out_copy(h):
        cols = pl.ds(pl.multiple_of(h * wide, HEAD), wide)
        return pltpu.make_async_copy(o_v.at[:, :, cols], o_hbm.at[0, :, :, cols], lo_sem.at[h])

    def wait_prior(j):
        @pl.when((me > 0) & jnp.logical_not(front))
        def _():
            p_copy(j).wait_recv()

        @pl.when(front)
        def _():
            q_copy(j).wait_recv()
            f_copy(j).wait_recv()
            prior[j] = (
                behind[j] + kq[j].astype(jnp.float32) + fr[j].astype(jnp.float32)
            ).astype(jnp.bfloat16)

    def weigh(h):
        wait_prior(2 * h)
        for s in range(slots):
            here = slice(s * tok, (s + 1) * tok)
            keys = jnp.concatenate([prior[2 * h, here], kv[2 * h, here]], axis=0)
            allowed = key_pos >= start_s[s]
            for q in range(q_per_kv):
                cols = pl.ds(pl.multiple_of((h * q_per_kv + q) * HEAD, HEAD), HEAD)
                both = lax.dot_general(
                    q_v[s, :, cols], keys, (((1,), (1,)), ((), ())),
                    preferred_element_type=jnp.float32,
                )
                scores = jnp.where(own, both[:, tok:], both[:, :tok]) * HEAD ** (-0.5)
                scores = jnp.where(allowed, scores, -1e30)
                maxima = jnp.max(scores, axis=-1, keepdims=True)
                exponent = jnp.exp(scores - maxima)
                sums = jnp.sum(exponent, axis=-1, keepdims=True)
                soft = exponent * (1.0 / sums)
                weights[s, q, :, 0:tok] = jnp.where(own, 0.0, soft).astype(jnp.bfloat16)
                weights[s, q, :, tok:] = jnp.where(own, soft, 0.0).astype(jnp.bfloat16)

    def mix(h):
        wait_prior(2 * h + 1)
        for s in range(slots):
            here = slice(s * tok, (s + 1) * tok)
            values = jnp.concatenate([prior[2 * h + 1, here], kv[2 * h + 1, here]], axis=0)
            for q in range(q_per_kv):
                cols = pl.ds(pl.multiple_of((h * q_per_kv + q) * HEAD, HEAD), HEAD)
                o_v[s, :, cols] = dot(weights[s, q], values).astype(jnp.bfloat16)
        out_copy(h).start()

    @pl.when(hub)
    def _():
        first_late = jnp.where(far, EARLY // 2, heads - LAG)

        def step(j):
            meet_hub(j)

            @pl.when(j + LEAD < pieces)
            def _():
                pass_leaf(j + LEAD)

            @pl.when(j > 0)
            def _():
                settle_hub(j - 1)

            @pl.when((j % 2 == 1) & (j > 2 * LAG) & (j // 2 - LAG < first_late))
            def _():
                weigh(j // 2 - LAG)
                mix(j // 2 - LAG)

        loop(0, pieces, step)
        settle_hub(pieces - 1)

        def rest(h):
            weigh(h)
            mix(h)

        loop(first_late, heads, rest)

    @pl.when(leaf)
    def _():
        def step(h):
            meet_leaf(2 * h)

            @pl.when(h > 0)
            def _():
                mix(h - 1)

            weigh(h)
            meet_leaf(2 * h + 1)

        loop(0, pieces, gather_leaf)
        loop(0, heads, step)
        mix(heads - 1)

    def drain(j):
        y_copy(j).wait_send()

        @pl.when((me < n - 1) & jnp.logical_not(cross & (j % 2 == 0)) & jnp.logical_not(rear))
        def _():
            p_copy(j).wait_send()

        @pl.when(base)
        def _():
            q_copy(j).wait_send()

        @pl.when(mate)
        def _():
            f_copy(j).wait_send()

        @pl.when((cross & (j % 2 == 0)) | rear)
        def _():
            e_copy(j).wait_send()

        @pl.when(relay & (j % 2 == 0))
        def _():
            r_copy(j).wait_send()

        @pl.when(hub)
        def _():
            w_pair(j, 0).wait_send()
            l_copy(j).wait_send()
            z_copy(j).wait_send()
            for d in span:
                w_hub(j, 0, d, grp).wait_send()
                w_hub(j, 1, d, grp).wait_send()
                if keep:
                    w_keep(j, d).wait_send()

        @pl.when(leaf)
        def _():
            w_pair(j, 1).wait_send()

    loop(0, pieces, drain)
    for s in range(slots):
        for g in range(groups):
            for k in range(2):
                x_y(s, g, k).wait_send()

    @pl.when(leaf)
    def _():
        for p in range(2 * slots):
            for d in span:
                for k in range(2):
                    x_z(p, d, k).wait_send()

    for h in range(heads):
        out_copy(h).wait()


def body(tokens, queries, gains, key_weight, value_weight, lengths):
    n = lax.axis_size(AXIS)
    _, slots, tok, depth = tokens.shape
    _, rows, key_width = key_weight.shape
    heads = key_width // HEAD
    pieces = 2 * heads
    groups = n // 4
    total = slots * tok
    keep = rows // 2 // HEAD * HEAD
    bf, f32 = jnp.bfloat16, jnp.float32
    any_spec = pl.BlockSpec(memory_space=pl.ANY)
    vmem_spec = pl.BlockSpec(memory_space=pltpu.VMEM)
    dma = pltpu.SemaphoreType.DMA
    fan = groups - 1
    return pl.pallas_call(
        functools.partial(kernel, n, keep),
        out_shape=jax.ShapeDtypeStruct(queries.shape, bf),
        in_specs=[any_spec, any_spec, vmem_spec, any_spec, any_spec, vmem_spec],
        out_specs=any_spec,
        scratch_shapes=[
            pltpu.VMEM((slots, tok, depth), bf),
            pltpu.VMEM(queries.shape[1:], bf),
            pltpu.VMEM(queries.shape[1:], bf),
            pltpu.VMEM((pieces, groups, 2, rows, HEAD), bf),
            pltpu.VMEM((groups, 2, 2 * total, rows), bf),
            pltpu.VMEM((groups, 2, total, rows), bf),
            pltpu.VMEM((groups, 2, 2 * total, rows), bf),
            pltpu.VMEM((pieces, 2 * total, HEAD), f32),
            pltpu.VMEM((pieces, total, HEAD), bf),
            pltpu.VMEM((pieces, total, HEAD), bf),
            pltpu.VMEM((pieces, total, HEAD), bf),
            pltpu.VMEM((pieces, total, HEAD), bf),
            pltpu.VMEM((pieces, total, HEAD), bf),
            pltpu.VMEM((pieces, total, HEAD), bf),
            pltpu.VMEM((pieces, total, HEAD), bf),
            pltpu.VMEM((pieces, total, HEAD), bf),
            pltpu.VMEM((pieces, total, HEAD), bf),
            pltpu.VMEM((pieces, total, HEAD), bf),
            pltpu.VMEM((pieces, total, HEAD), bf),
            pltpu.VMEM((pieces, total, HEAD), bf),
            pltpu.VMEM((pieces, total, HEAD), bf),
            pltpu.VMEM((pieces, total, HEAD), bf),
            pltpu.VMEM((pieces, total, HEAD), f32),
            pltpu.VMEM((pieces, total, HEAD), f32),
            pltpu.VMEM((2 * total, HEAD), f32),
            pltpu.VMEM((slots, queries.shape[-1] // key_width, tok, 2 * tok), bf),
            pltpu.VMEM((slots, tok, HEAD), jnp.int32),
            dma((pieces,)), dma((slots,)), dma, dma((heads,)),
            dma((pieces,)), dma((pieces,)),
            dma((pieces, 2, fan)), dma((pieces, 2, groups)),
            dma((pieces, fan)), dma((pieces, fan)),
            dma((slots, groups, 2)), dma((slots, groups, 2)),
            dma((2 * slots, fan, 2)), dma((2 * slots, fan, 2)),
            dma((pieces,)), dma((pieces,)),
            dma((pieces,)), dma((pieces,)),
            dma((pieces,)), dma((pieces,)),
            dma((pieces,)), dma((pieces,)),
            dma((pieces,)), dma((pieces,)), dma((pieces,)), dma((pieces,)),
            dma((pieces,)), dma((pieces,)), dma((pieces,)),
        ],
        compiler_params=pltpu.CompilerParams(
            collective_id=0, has_side_effects=True, vmem_limit_bytes=60 * 1024 * 1024
        ),
    )(tokens, queries, gains, key_weight, value_weight, lengths)


def solution(mesh):
    return jax.shard_map(
        body,
        mesh=mesh,
        in_specs=(
            P("section", None, "fsdp", None),
            P("section", None, "fsdp", None),
            P("section", None),
            P("section", "fsdp", None),
            P("section", "fsdp", None),
            P(),
        ),
        out_specs=P("section", None, "fsdp", None),
        check_vma=False,
    )
```

```python
import functools

import jax
import jax.numpy as jnp
from jax import lax
from jax.experimental import pallas as pl
from jax.experimental.pallas import tpu as pltpu
from jax.sharding import PartitionSpec as P

HEAD = 128
AXIS = "fsdp"
LEAD = 2
LAG = 2
EARLY = 0


def kernel(
    n, keep,
    x_hbm, q_hbm, gain_ref, kw_hbm, vw_hbm, len_ref, o_hbm,
    x_v, q_v, o_v, wbuf, xs, sx, lx, acc, ls, lr, zs, zr, ys, yr, es, er, fs, fr, kv, kx, kq, prior, side, behind, part_s, us, ua, ub, weights, start_s,
    lw_sem, lx_sem, lq_sem, lo_sem,
    wz_s, wz_r, wh_s, wh_r, wk_s, wk_r, xy_s, xy_r, xz_s, xz_r,
    l_s, l_r, z_s, z_r, y_s, y_r, e_s, e_r, f_s, f_r, p_s, p_r, q_s, q_r, r_s, u_s, u_r,
):
    slots, tok, depth = x_v.shape
    pieces, groups, _, rows, _ = wbuf.shape
    heads = pieces // 2
    total = slots * tok
    q_per_kv = q_v.shape[2] // (heads * HEAD)
    me = lax.axis_index(AXIS)
    bit = me % 2
    cls = (me // 2) % 2
    grp = me // 4
    leaf = cls == grp % 2
    hub = jnp.logical_not(leaf)
    kind = jnp.where(leaf, 1, 0)
    y_peer = me + 1 - 2 * bit
    z_peer = me + 2 - 4 * cls
    diagonal = z_peer + 1 - 2 * bit
    final = pieces - 1
    right = lax.rem(me + 1, n)
    left = lax.rem(me + n - 1, n)
    others = [lax.rem(grp + d, groups) for d in range(1, groups)]
    span = range(len(others))
    cross = (me % 4 == 3) & (grp % 2 == 0) & (me < n - 1)
    relay = (me % 4 == 2) & (grp % 2 == 0) & (me < n - 2)
    far = (me % 4 == 0) & (grp % 2 == 1)
    base = (me % 4 == 0) & (grp % 2 == 0)
    rear = (me % 4 == 1) & (grp % 2 == 0)
    front = (me % 4 == 2) & (grp % 2 == 0)
    mate = (me % 4 == 3) & (grp % 2 == 0)

    def hub_of(g):
        return 4 * g + 2 * (1 - g % 2) + bit

    def load_w(j):
        w = vw_hbm if j % 2 else kw_hbm
        cols = pl.ds((j // 2) * HEAD, HEAD)
        return pltpu.make_async_copy(w.at[0, :, cols], wbuf.at[j, grp, kind], lw_sem.at[j])

    x_loads = [pltpu.make_async_copy(x_hbm.at[0, s], x_v.at[s], lx_sem.at[s]) for s in range(slots)]
    q_load = pltpu.make_async_copy(q_hbm.at[0], q_v, lq_sem)
    w_loads = [load_w(j) for j in range(pieces)]
    for copy in w_loads[:2] + x_loads[:1] + w_loads[2:] + x_loads[1:] + [q_load]:
        copy.start()

    barrier = pltpu.get_barrier_semaphore()

    def greet(peer):
        pl.semaphore_signal(barrier, inc=1, device_id={AXIS: peer}, device_id_type=pl.DeviceIdType.MESH)

    greet(y_peer)
    greet(z_peer)
    greet(diagonal)

    @pl.when(hub)
    def _():
        for g in others:
            greet(hub_of(g))

    @pl.when(me < n - 1)
    def _():
        greet(right)

    @pl.when(relay)
    def _():
        greet(lax.rem(me + 2, n))

    @pl.when(far)
    def _():
        greet(me - 2)

    @pl.when(me > 0)
    def _():
        greet(left)

    prior[...] = jnp.zeros_like(prior)
    pl.semaphore_wait(
        barrier,
        3 + jnp.where(hub, len(others), 0) + jnp.where(me < n - 1, 1, 0) + jnp.where(me > 0, 1, 0)
        + jnp.where(relay, 1, 0) + jnp.where(far, 1, 0),
    )

    def remote(src, dst, send, recv, peer):
        return pltpu.make_async_remote_copy(
            src_ref=src, dst_ref=dst, send_sem=send, recv_sem=recv,
            device_id={AXIS: peer}, device_id_type=pl.DeviceIdType.MESH,
        )

    def w_pair(j, k):
        block = wbuf.at[j, grp, k]
        return remote(block, block, wz_s.at[j], wz_r.at[j], z_peer)

    def w_hub(j, k, d, g):
        block = wbuf.at[j, g, k]
        return remote(block, block, wh_s.at[j, k, d], wh_r.at[j, k, g], hub_of(others[d]))

    def w_keep(j, d):
        block = wbuf.at[j, others[d], 0, pl.ds(0, keep)]
        return remote(block, block, wk_s.at[j, d], wk_r.at[j, d], z_peer)

    def x_y(s, g, k):
        return remote(
            sx.at[g, k, pl.ds(s * tok, tok)], xs.at[g, k, pl.ds(total + s * tok, tok)],
            xy_s.at[s, g, k], xy_r.at[s, g, k], y_peer,
        )

    def x_z(p, d, k):
        skip = 0 if k else keep
        here = (others[d], k, pl.ds(p * tok, tok), pl.ds(skip, rows - skip))
        return remote(xs.at[here], lx.at[here], xz_s.at[p, d, k], xz_r.at[p, d, k], z_peer)

    def l_copy(j):
        return remote(ls.at[j], lr.at[j], l_s.at[j], l_r.at[j], y_peer)

    def z_copy(j):
        return remote(zs.at[j], zr.at[j], z_s.at[j], z_r.at[j], z_peer)

    def y_copy(j):
        return remote(ys.at[j], yr.at[j], y_s.at[j], y_r.at[j], y_peer)

    def e_copy(j):
        return remote(es.at[j], er.at[j], e_s.at[j], e_r.at[j], y_peer)

    def f_copy(j):
        return remote(fs.at[j], fr.at[j], f_s.at[j], f_r.at[j], y_peer)

    def q_copy(j):
        return remote(kx.at[j], kq.at[j], q_s.at[j], q_r.at[j], z_peer)

    def near(size):
        rows_of = pl.ds(0, size)
        return remote(us.at[rows_of], ua.at[rows_of], u_s.at[0], u_r.at[0], z_peer)

    def slant(first, size):
        return remote(
            us.at[pl.ds(first, size)], ub.at[pl.ds(0, size)], u_s.at[1], u_r.at[1], diagonal
        )

    def p_copy(j):
        return remote(kv.at[j], prior.at[j], p_s.at[j], p_r.at[j], right)

    def r_copy(j):
        return remote(kx.at[j], prior.at[j], r_s.at[j], p_r.at[j], lax.rem(me + 2, n))

    for j in range(pieces):
        w_loads[j].wait()

        @pl.when(hub)
        def _(j=j):
            w_pair(j, 0).start()
            for d in span:
                w_hub(j, 0, d, grp).start()

        if j < LEAD:
            @pl.when(leaf)
            def _(j=j):
                w_pair(j, 1).start()

    block_rows = 16

    def norm_block(s, r):
        here = pl.ds(pl.multiple_of(r * block_rows, block_rows), block_rows)
        there = pl.ds(pl.multiple_of(s * tok + r * block_rows, block_rows), block_rows)
        squares = jnp.zeros((block_rows, 1), jnp.float32)
        step = 4 * HEAD
        for i in range(depth // step):
            piece = x_v[s, here, i * step:(i + 1) * step].astype(jnp.float32)
            squares = squares + jnp.sum(piece * piece, axis=-1, keepdims=True)
        inverse = lax.rsqrt(squares / depth + 1e-05)
        for g in range(groups):
            for k in range(2):
                line = g % 2 if k else 1 - g % 2
                for mine in (False, True):
                    first = (4 * g + 2 * line + (bit if mine else 1 - bit)) * rows
                    cols = pl.ds(pl.multiple_of(first, HEAD), rows)
                    value = x_v[s, here, cols].astype(jnp.float32) * inverse
                    value = (value * gain_ref[0:1, cols].astype(jnp.float32)).astype(jnp.bfloat16)
                    if mine:
                        xs[g, k, there, :] = value
                    else:
                        sx[g, k, there, :] = value

    for s in range(slots):
        x_loads[s].wait()

        def norm_step(r, carry, s=s):
            norm_block(s, r)
            return carry

        lax.fori_loop(0, tok // block_rows, norm_step, 0)
        for g in others + [grp]:
            for k in range(2):
                x_y(s, g, k).start()

        @pl.when(leaf)
        def _(s=s):
            for d in span:
                for k in range(2):
                    x_z(s, d, k).start()

    docs = len_ref.shape[1]
    rowi = lax.broadcasted_iota(jnp.int32, (docs, docs), 0)
    coli = lax.broadcasted_iota(jnp.int32, (docs, docs), 1)
    pos = lax.broadcasted_iota(jnp.int32, (tok, 1), 0) + me * tok
    for s in range(slots):
        lens = jnp.broadcast_to(len_ref[s:s + 1, :], (docs, docs))
        bounds = jnp.sum(jnp.where(coli <= rowi, lens, 0), axis=1, keepdims=True)
        bound_row = jnp.sum(jnp.where(coli == rowi, bounds, 0), axis=0, keepdims=True)
        start = jnp.max(jnp.where(bound_row <= pos, bound_row, 0), axis=1, keepdims=True)
        start_s[s] = jnp.broadcast_to(start, (tok, HEAD))
    q_load.wait()

    def dot(a, b):
        return jnp.dot(a, b, preferred_element_type=jnp.float32)

    def loop(lo, hi, step):
        def run(j, carry):
            step(j)
            return carry

        lax.fori_loop(lo, hi, run, 0)

    def take_hub(j):
        for d in span:
            w_hub(j, 0, d, others[d]).wait_recv()
            if keep:
                w_keep(j, d).start()

    def pass_leaf(j):
        w_pair(j, 1).wait_recv()
        for d in span:
            w_hub(j, 1, d, grp).start()

    @pl.when(hub)
    def _():
        loop(0, pieces // 2, take_hub)
        loop(0, LEAD, pass_leaf)
        loop(pieces // 2, pieces, take_hub)
        for s in range(slots):
            for g in others + [grp]:
                for k in range(2):
                    x_y(s, g, k).wait_recv()

        def first(j):
            value = dot(xs[grp, 0], wbuf[j, grp, 0])
            for g in others:
                value = value + dot(xs[g, 0], wbuf[j, g, 0])
            acc[j] = value

        loop(0, pieces, first)
        for p in range(2 * slots):
            for d in span:
                for k in range(2):
                    x_z(p, d, k).wait_recv()

    @pl.when(leaf)
    def _():
        for s in range(slots):
            for d in span:
                for k in range(2):
                    x_y(s, others[d], k).wait_recv()
                    x_z(slots + s, d, k).start()

        def send_w(j):
            w_pair(j, 1).start()

        loop(LEAD, pieces, send_w)
        for s in range(slots):
            for k in range(2):
                x_y(s, grp, k).wait_recv()

        def first(j):
            w_pair(j, 0).wait_recv()
            acc[j] = dot(xs[grp, 0], wbuf[j, grp, 0]) + dot(xs[grp, 1], wbuf[j, grp, 1])

        loop(0, pieces, first)
        def second(j):
            value = acc[j]
            if keep:
                for d in span:
                    w_keep(j, d).wait_recv()
                    value = value + dot(
                        xs[others[d], 0, :, 0:keep], wbuf[j, others[d], 0, 0:keep]
                    )
                acc[j] = value
            ys[j] = value[total:].astype(jnp.bfloat16)
            y_copy(j).start()

            @pl.when(rear | ((bit == 0) & (j == final)))
            def _():
                es[j] = value[:total].astype(jnp.bfloat16)
                e_copy(j).start()

        loop(0, pieces, second)

    def send_prior(j):
        @pl.when((me < n - 1) & jnp.logical_not(cross) & jnp.logical_not(rear | (leaf & (bit == 0) & (j == final))))
        def _():
            p_copy(j).start()

    def cross_over(j):
        @pl.when(cross & (j % 2 == 1))
        def _():
            p_copy(j).start()

        @pl.when(relay & (j % 2 == 0))
        def _():
            r_copy(j).start()

    held = pieces - LEAD - 2

    def meet_hub(j, last):
        part = jnp.zeros((2 * total, HEAD), jnp.float32)
        for g in others:
            part = part + dot(lx[g, 0, :, keep:], wbuf[j, g, 0, keep:])
        part_s[...] = part
        acc[j] = acc[j] + dot(xs[grp, 1], wbuf[j, grp, 1])
        for d in span:
            w_hub(j, 1, d, others[d]).wait_recv()
        part = part_s[...]
        for g in others:
            part = part + dot(lx[g, 1], wbuf[j, g, 1])
        if last:
            us[...] = part.astype(jnp.bfloat16)

            @pl.when(bit == 0)
            def _():
                slant(0, 2 * total).start()
                near(total).start()

            @pl.when(bit == 1)
            def _():
                near(2 * total).start()
                slant(total, total).start()
        else:
            ls[j] = part[total:].astype(jnp.bfloat16)
            l_copy(j).start()
        value = acc[j]
        for g in others:
            value = value + dot(xs[g, 1], wbuf[j, g, 1])
        ys[j] = value[total:].astype(jnp.bfloat16)
        y_copy(j).start()
        acc[j, 0:total] = value[:total]
        acc[j, total:] = part[:total]

        @pl.when(mate)
        def _():
            fs[j] = part[:total].astype(jnp.bfloat16)
            f_copy(j).start()

        @pl.when(cross & (j % 2 == 0))
        def _():
            es[j] = value[:total].astype(jnp.bfloat16)
            e_copy(j).start()

        @pl.when(front)
        def _():
            behind[j] = part[total:]

        @pl.when(relay & (j % 2 == 0))
        def _():
            side[j] = value[total:]

    def settle_hub(j, last=False):
        if not last:
            l_copy(j).wait_recv()
            zs[j] = (acc[j, total:] + lr[j].astype(jnp.float32)).astype(jnp.bfloat16)
            z_copy(j).start()
        y_copy(j).wait_recv()
        kv[j] = (acc[j, 0:total] + yr[j].astype(jnp.float32)).astype(jnp.bfloat16)
        send_prior(j)

        @pl.when(relay & (j % 2 == 0))
        def _():
            e_copy(j).wait_recv()
            kx[j] = (side[j] + er[j].astype(jnp.float32)).astype(jnp.bfloat16)

        @pl.when((j < EARLY) | (j > held))
        def _():
            cross_over(j)

        @pl.when(j == held)
        def _():
            loop(EARLY, held + 1, cross_over)

    def gather_leaf(j):
        y_copy(j).wait_recv()
        value = acc[j, 0:total] + yr[j].astype(jnp.float32)
        acc[j, 0:total] = value

        @pl.when((bit == 1) & (j == final))
        def _():
            e_copy(j).wait_recv()
            acc[j, total:] = acc[j, total:] + er[j].astype(jnp.float32)

        @pl.when(base)
        def _():
            e_copy(j).wait_recv()
            kx[j] = (acc[j, total:] + er[j].astype(jnp.float32)).astype(jnp.bfloat16)
            q_copy(j).start()

    def meet_leaf(j):
        z_copy(j).wait_recv()
        kv[j] = (acc[j, 0:total] + zr[j].astype(jnp.float32)).astype(jnp.bfloat16)
        send_prior(j)

    def last_leaf():
        def sums(mine, other):
            value = acc[final, mine:mine + total] + ua[mine:mine + total].astype(jnp.float32)
            return (value + ub[other:other + total].astype(jnp.float32)).astype(jnp.bfloat16)

        @pl.when(bit == 0)
        def _():
            near(total).wait_recv()
            slant(total, total).wait_recv()
            kv[final] = sums(0, 0)

        @pl.when(bit == 1)
        def _():
            near(2 * total).wait_recv()
            slant(0, 2 * total).wait_recv()
            kv[final] = sums(0, total)
            prior[final] = sums(total, 0)

        send_prior(final)

    lane = lax.broadcasted_iota(jnp.int32, (tok, tok), 1)
    own = lane <= lax.broadcasted_iota(jnp.int32, (tok, tok), 0)
    key_pos = lane + jnp.where(own, me, me - 1) * tok
    wide = q_per_kv * HEAD

    def out_copy(h):
        cols = pl.ds(pl.multiple_of(h * wide, HEAD), wide)
        return pltpu.make_async_copy(o_v.at[:, :, cols], o_hbm.at[0, :, :, cols], lo_sem.at[h])

    def wait_prior(j):
        @pl.when((me > 0) & jnp.logical_not(front | (leaf & (bit == 1) & (j == final))))
        def _():
            p_copy(j).wait_recv()

        @pl.when(front)
        def _():
            q_copy(j).wait_recv()
            f_copy(j).wait_recv()
            prior[j] = (
                behind[j] + kq[j].astype(jnp.float32) + fr[j].astype(jnp.float32)
            ).astype(jnp.bfloat16)

    def weigh(h):
        wait_prior(2 * h)
        for s in range(slots):
            here = slice(s * tok, (s + 1) * tok)
            keys = jnp.concatenate([prior[2 * h, here], kv[2 * h, here]], axis=0)
            allowed = key_pos >= start_s[s]
            for q in range(q_per_kv):
                cols = pl.ds(pl.multiple_of((h * q_per_kv + q) * HEAD, HEAD), HEAD)
                both = lax.dot_general(
                    q_v[s, :, cols], keys, (((1,), (1,)), ((), ())),
                    preferred_element_type=jnp.float32,
                )
                scores = jnp.where(own, both[:, tok:], both[:, :tok]) * HEAD ** (-0.5)
                scores = jnp.where(allowed, scores, -1e30)
                maxima = jnp.max(scores, axis=-1, keepdims=True)
                exponent = jnp.exp(scores - maxima)
                sums = jnp.sum(exponent, axis=-1, keepdims=True)
                soft = exponent * (1.0 / sums)
                weights[s, q, :, 0:tok] = jnp.where(own, 0.0, soft).astype(jnp.bfloat16)
                weights[s, q, :, tok:] = jnp.where(own, soft, 0.0).astype(jnp.bfloat16)

    def mix(h):
        wait_prior(2 * h + 1)
        for s in range(slots):
            here = slice(s * tok, (s + 1) * tok)
            values = jnp.concatenate([prior[2 * h + 1, here], kv[2 * h + 1, here]], axis=0)
            for q in range(q_per_kv):
                cols = pl.ds(pl.multiple_of((h * q_per_kv + q) * HEAD, HEAD), HEAD)
                o_v[s, :, cols] = dot(weights[s, q], values).astype(jnp.bfloat16)
        out_copy(h).start()

    @pl.when(hub)
    def _():
        first_late = jnp.where(far, EARLY // 2, heads - LAG)

        def step(j):
            meet_hub(j, False)

            @pl.when(j + LEAD < pieces)
            def _():
                pass_leaf(j + LEAD)

            @pl.when(j > 0)
            def _():
                settle_hub(j - 1)

            @pl.when((j % 2 == 1) & (j > 2 * LAG) & (j // 2 - LAG < first_late))
            def _():
                weigh(j // 2 - LAG)
                mix(j // 2 - LAG)

        loop(0, final, step)

        @pl.when(first_late == heads - LAG)
        def _():
            weigh(heads - 1 - LAG)
            mix(heads - 1 - LAG)

        settle_hub(final - 1)
        meet_hub(final, True)
        settle_hub(final, True)

        def rest(h):
            weigh(h)
            mix(h)

        loop(first_late, heads, rest)

    @pl.when(leaf)
    def _():
        def step(h):
            meet_leaf(2 * h)

            @pl.when(h > 0)
            def _():
                mix(h - 1)

            weigh(h)

            @pl.when(2 * h + 1 < final)
            def _():
                meet_leaf(2 * h + 1)

        loop(0, pieces, gather_leaf)
        loop(0, heads, step)
        last_leaf()
        mix(heads - 1)

    def drain(j):
        y_copy(j).wait_send()

        @pl.when((me < n - 1) & jnp.logical_not(
            (cross & (j % 2 == 0)) | rear | (leaf & (bit == 0) & (j == final))
        ))
        def _():
            p_copy(j).wait_send()

        @pl.when(base)
        def _():
            q_copy(j).wait_send()

        @pl.when(mate)
        def _():
            f_copy(j).wait_send()

        @pl.when((cross & (j % 2 == 0)) | rear | (leaf & (bit == 0) & (j == final)))
        def _():
            e_copy(j).wait_send()

        @pl.when(relay & (j % 2 == 0))
        def _():
            r_copy(j).wait_send()

        @pl.when(hub)
        def _():
            w_pair(j, 0).wait_send()

            @pl.when(j < final)
            def _():
                l_copy(j).wait_send()
                z_copy(j).wait_send()

            for d in span:
                w_hub(j, 0, d, grp).wait_send()
                w_hub(j, 1, d, grp).wait_send()
                if keep:
                    w_keep(j, d).wait_send()

        @pl.when(leaf)
        def _():
            w_pair(j, 1).wait_send()

    loop(0, pieces, drain)

    @pl.when(hub & (bit == 0))
    def _():
        slant(0, 2 * total).wait_send()
        near(total).wait_send()

    @pl.when(hub & (bit == 1))
    def _():
        near(2 * total).wait_send()
        slant(total, total).wait_send()

    for s in range(slots):
        for g in range(groups):
            for k in range(2):
                x_y(s, g, k).wait_send()

    @pl.when(leaf)
    def _():
        for p in range(2 * slots):
            for d in span:
                for k in range(2):
                    x_z(p, d, k).wait_send()

    for h in range(heads):
        out_copy(h).wait()


def body(tokens, queries, gains, key_weight, value_weight, lengths):
    n = lax.axis_size(AXIS)
    _, slots, tok, depth = tokens.shape
    _, rows, key_width = key_weight.shape
    heads = key_width // HEAD
    pieces = 2 * heads
    groups = n // 4
    total = slots * tok
    keep = rows // 2 // HEAD * HEAD
    bf, f32 = jnp.bfloat16, jnp.float32
    any_spec = pl.BlockSpec(memory_space=pl.ANY)
    vmem_spec = pl.BlockSpec(memory_space=pltpu.VMEM)
    dma = pltpu.SemaphoreType.DMA
    fan = groups - 1
    return pl.pallas_call(
        functools.partial(kernel, n, keep),
        out_shape=jax.ShapeDtypeStruct(queries.shape, bf),
        in_specs=[any_spec, any_spec, vmem_spec, any_spec, any_spec, vmem_spec],
        out_specs=any_spec,
        scratch_shapes=[
            pltpu.VMEM((slots, tok, depth), bf),
            pltpu.VMEM(queries.shape[1:], bf),
            pltpu.VMEM(queries.shape[1:], bf),
            pltpu.VMEM((pieces, groups, 2, rows, HEAD), bf),
            pltpu.VMEM((groups, 2, 2 * total, rows), bf),
            pltpu.VMEM((groups, 2, total, rows), bf),
            pltpu.VMEM((groups, 2, 2 * total, rows), bf),
            pltpu.VMEM((pieces, 2 * total, HEAD), f32),
            pltpu.VMEM((pieces, total, HEAD), bf),
            pltpu.VMEM((pieces, total, HEAD), bf),
            pltpu.VMEM((pieces, total, HEAD), bf),
            pltpu.VMEM((pieces, total, HEAD), bf),
            pltpu.VMEM((pieces, total, HEAD), bf),
            pltpu.VMEM((pieces, total, HEAD), bf),
            pltpu.VMEM((pieces, total, HEAD), bf),
            pltpu.VMEM((pieces, total, HEAD), bf),
            pltpu.VMEM((pieces, total, HEAD), bf),
            pltpu.VMEM((pieces, total, HEAD), bf),
            pltpu.VMEM((pieces, total, HEAD), bf),
            pltpu.VMEM((pieces, total, HEAD), bf),
            pltpu.VMEM((pieces, total, HEAD), bf),
            pltpu.VMEM((pieces, total, HEAD), bf),
            pltpu.VMEM((pieces, total, HEAD), f32),
            pltpu.VMEM((pieces, total, HEAD), f32),
            pltpu.VMEM((2 * total, HEAD), f32),
            pltpu.VMEM((2 * total, HEAD), bf),
            pltpu.VMEM((2 * total, HEAD), bf),
            pltpu.VMEM((2 * total, HEAD), bf),
            pltpu.VMEM((slots, queries.shape[-1] // key_width, tok, 2 * tok), bf),
            pltpu.VMEM((slots, tok, HEAD), jnp.int32),
            dma((pieces,)), dma((slots,)), dma, dma((heads,)),
            dma((pieces,)), dma((pieces,)),
            dma((pieces, 2, fan)), dma((pieces, 2, groups)),
            dma((pieces, fan)), dma((pieces, fan)),
            dma((slots, groups, 2)), dma((slots, groups, 2)),
            dma((2 * slots, fan, 2)), dma((2 * slots, fan, 2)),
            dma((pieces,)), dma((pieces,)),
            dma((pieces,)), dma((pieces,)),
            dma((pieces,)), dma((pieces,)),
            dma((pieces,)), dma((pieces,)),
            dma((pieces,)), dma((pieces,)), dma((pieces,)), dma((pieces,)),
            dma((pieces,)), dma((pieces,)), dma((pieces,)),
            dma((2,)), dma((2,)),
        ],
        compiler_params=pltpu.CompilerParams(
            collective_id=0, has_side_effects=True, vmem_limit_bytes=60 * 1024 * 1024
        ),
    )(tokens, queries, gains, key_weight, value_weight, lengths)


def solution(mesh):
    return jax.shard_map(
        body,
        mesh=mesh,
        in_specs=(
            P("section", None, "fsdp", None),
            P("section", None, "fsdp", None),
            P("section", None),
            P("section", "fsdp", None),
            P("section", "fsdp", None),
            P(),
        ),
        out_specs=P("section", None, "fsdp", None),
        check_vma=False,
    )
```

```python
import functools

import jax
import jax.numpy as jnp
from jax import lax
from jax.experimental import pallas as pl
from jax.experimental.pallas import tpu as pltpu
from jax.sharding import PartitionSpec as P

HEAD = 128
AXIS = "fsdp"
LEAD = 2
LAG = 2
EARLY = 0


def kernel(
    n, keep,
    x_hbm, q_hbm, gain_ref, kw_hbm, vw_hbm, len_ref, o_hbm,
    x_v, q_v, o_v, wbuf, xs, sx, lx, acc, ls, lr, zs, zr, ys, yr, es, er, fs, fr, kv, kx, kq, prior, side, behind, part_s, us, ua, ub, weights, start_s,
    lw_sem, lx_sem, lq_sem, lo_sem,
    wz_s, wz_r, wh_s, wh_r, wk_s, wk_r, xy_s, xy_r, xz_s, xz_r,
    l_s, l_r, z_s, z_r, y_s, y_r, e_s, e_r, f_s, f_r, p_s, p_r, q_s, q_r, r_s, u_s, u_r,
):
    slots, tok, depth = x_v.shape
    pieces, groups, _, rows, _ = wbuf.shape
    heads = pieces // 2
    total = slots * tok
    q_per_kv = q_v.shape[2] // (heads * HEAD)
    me = lax.axis_index(AXIS)
    bit = me % 2
    cls = (me // 2) % 2
    grp = me // 4
    leaf = cls == grp % 2
    hub = jnp.logical_not(leaf)
    kind = jnp.where(leaf, 1, 0)
    y_peer = me + 1 - 2 * bit
    z_peer = me + 2 - 4 * cls
    diagonal = z_peer + 1 - 2 * bit
    final = pieces - 1
    right = lax.rem(me + 1, n)
    left = lax.rem(me + n - 1, n)
    others = [lax.rem(grp + d, groups) for d in range(1, groups)]
    span = range(len(others))
    cross = (me % 4 == 3) & (grp % 2 == 0) & (me < n - 1)
    relay = (me % 4 == 2) & (grp % 2 == 0) & (me < n - 2)
    far = (me % 4 == 0) & (grp % 2 == 1)
    base = (me % 4 == 0) & (grp % 2 == 0)
    rear = (me % 4 == 1) & (grp % 2 == 0)
    front = (me % 4 == 2) & (grp % 2 == 0)
    mate = (me % 4 == 3) & (grp % 2 == 0)

    def hub_of(g):
        return 4 * g + 2 * (1 - g % 2) + bit

    def load_w(j):
        w = vw_hbm if j % 2 else kw_hbm
        cols = pl.ds((j // 2) * HEAD, HEAD)
        return pltpu.make_async_copy(w.at[0, :, cols], wbuf.at[j, grp, kind], lw_sem.at[j])

    x_loads = [pltpu.make_async_copy(x_hbm.at[0, s], x_v.at[s], lx_sem.at[s]) for s in range(slots)]
    q_load = pltpu.make_async_copy(q_hbm.at[0], q_v, lq_sem)
    w_loads = [load_w(j) for j in range(pieces)]
    for copy in w_loads[:2] + x_loads[:1] + w_loads[2:] + x_loads[1:] + [q_load]:
        copy.start()

    barrier = pltpu.get_barrier_semaphore()

    def greet(peer):
        pl.semaphore_signal(barrier, inc=1, device_id={AXIS: peer}, device_id_type=pl.DeviceIdType.MESH)

    greet(y_peer)
    greet(z_peer)
    greet(diagonal)

    @pl.when(hub)
    def _():
        for g in others:
            greet(hub_of(g))

    @pl.when(me < n - 1)
    def _():
        greet(right)

    @pl.when(relay)
    def _():
        greet(lax.rem(me + 2, n))

    @pl.when(far)
    def _():
        greet(me - 2)

    @pl.when(me > 0)
    def _():
        greet(left)

    prior[...] = jnp.zeros_like(prior)
    pl.semaphore_wait(
        barrier,
        3 + jnp.where(hub, len(others), 0) + jnp.where(me < n - 1, 1, 0) + jnp.where(me > 0, 1, 0)
        + jnp.where(relay, 1, 0) + jnp.where(far, 1, 0),
    )

    def remote(src, dst, send, recv, peer):
        return pltpu.make_async_remote_copy(
            src_ref=src, dst_ref=dst, send_sem=send, recv_sem=recv,
            device_id={AXIS: peer}, device_id_type=pl.DeviceIdType.MESH,
        )

    def w_pair(j, k):
        block = wbuf.at[j, grp, k]
        return remote(block, block, wz_s.at[j], wz_r.at[j], z_peer)

    def w_hub(j, k, d, g):
        block = wbuf.at[j, g, k]
        return remote(block, block, wh_s.at[j, k, d], wh_r.at[j, k, g], hub_of(others[d]))

    def w_keep(j, d):
        block = wbuf.at[j, others[d], 0, pl.ds(0, keep)]
        return remote(block, block, wk_s.at[j, d], wk_r.at[j, d], z_peer)

    def x_y(s, g, k):
        return remote(
            sx.at[g, k, pl.ds(s * tok, tok)], xs.at[g, k, pl.ds(total + s * tok, tok)],
            xy_s.at[s, g, k], xy_r.at[s, g, k], y_peer,
        )

    def x_z(p, d, k):
        skip = 0 if k else keep
        here = (others[d], k, pl.ds(p * tok, tok), pl.ds(skip, rows - skip))
        return remote(xs.at[here], lx.at[here], xz_s.at[p, d, k], xz_r.at[p, d, k], z_peer)

    def l_copy(j):
        return remote(ls.at[j], lr.at[j], l_s.at[j], l_r.at[j], y_peer)

    def z_copy(j):
        return remote(zs.at[j], zr.at[j], z_s.at[j], z_r.at[j], z_peer)

    def y_copy(j):
        return remote(ys.at[j], yr.at[j], y_s.at[j], y_r.at[j], y_peer)

    def e_copy(j):
        return remote(es.at[j], er.at[j], e_s.at[j], e_r.at[j], y_peer)

    def f_copy(j):
        return remote(fs.at[j], fr.at[j], f_s.at[j], f_r.at[j], y_peer)

    def q_copy(j):
        return remote(kx.at[j], kq.at[j], q_s.at[j], q_r.at[j], z_peer)

    def near(size):
        rows_of = pl.ds(0, size)
        return remote(us.at[rows_of], ua.at[rows_of], u_s.at[0], u_r.at[0], z_peer)

    def slant(first, size):
        return remote(
            us.at[pl.ds(first, size)], ub.at[pl.ds(0, size)], u_s.at[1], u_r.at[1], diagonal
        )

    def p_copy(j):
        return remote(kv.at[j], prior.at[j], p_s.at[j], p_r.at[j], right)

    def r_copy(j):
        return remote(kx.at[j], prior.at[j], r_s.at[j], p_r.at[j], lax.rem(me + 2, n))

    for j in range(pieces):
        w_loads[j].wait()

        @pl.when(hub)
        def _(j=j):
            w_pair(j, 0).start()
            for d in span:
                w_hub(j, 0, d, grp).start()

        if j < LEAD:
            @pl.when(leaf)
            def _(j=j):
                w_pair(j, 1).start()

    block_rows = 16

    def norm_block(s, r):
        here = pl.ds(pl.multiple_of(r * block_rows, block_rows), block_rows)
        there = pl.ds(pl.multiple_of(s * tok + r * block_rows, block_rows), block_rows)
        squares = jnp.zeros((block_rows, 1), jnp.float32)
        step = 4 * HEAD
        for i in range(depth // step):
            piece = x_v[s, here, i * step:(i + 1) * step].astype(jnp.float32)
            squares = squares + jnp.sum(piece * piece, axis=-1, keepdims=True)
        inverse = lax.rsqrt(squares / depth + 1e-05)
        for g in range(groups):
            for k in range(2):
                line = g % 2 if k else 1 - g % 2
                for mine in (False, True):
                    first = (4 * g + 2 * line + (bit if mine else 1 - bit)) * rows
                    cols = pl.ds(pl.multiple_of(first, HEAD), rows)
                    value = x_v[s, here, cols].astype(jnp.float32) * inverse
                    value = (value * gain_ref[0:1, cols].astype(jnp.float32)).astype(jnp.bfloat16)
                    if mine:
                        xs[g, k, there, :] = value
                    else:
                        sx[g, k, there, :] = value

    for s in range(slots):
        x_loads[s].wait()

        def norm_step(r, carry, s=s):
            norm_block(s, r)
            return carry

        lax.fori_loop(0, tok // block_rows, norm_step, 0)
        for g in others + [grp]:
            for k in range(2):
                x_y(s, g, k).start()

        @pl.when(leaf)
        def _(s=s):
            for d in span:
                for k in range(2):
                    x_z(s, d, k).start()

    docs = len_ref.shape[1]
    rowi = lax.broadcasted_iota(jnp.int32, (docs, docs), 0)
    coli = lax.broadcasted_iota(jnp.int32, (docs, docs), 1)
    pos = lax.broadcasted_iota(jnp.int32, (tok, 1), 0) + me * tok
    for s in range(slots):
        lens = jnp.broadcast_to(len_ref[s:s + 1, :], (docs, docs))
        bounds = jnp.sum(jnp.where(coli <= rowi, lens, 0), axis=1, keepdims=True)
        bound_row = jnp.sum(jnp.where(coli == rowi, bounds, 0), axis=0, keepdims=True)
        start = jnp.max(jnp.where(bound_row <= pos, bound_row, 0), axis=1, keepdims=True)
        start_s[s] = jnp.broadcast_to(start, (tok, HEAD))
    q_load.wait()

    def dot(a, b):
        return jnp.dot(a, b, preferred_element_type=jnp.float32)

    def loop(lo, hi, step):
        def run(j, carry):
            step(j)
            return carry

        lax.fori_loop(lo, hi, run, 0)

    def take_hub(j):
        for d in span:
            w_hub(j, 0, d, others[d]).wait_recv()
            if keep:
                w_keep(j, d).start()

    def pass_leaf(j):
        w_pair(j, 1).wait_recv()
        for d in span:
            w_hub(j, 1, d, grp).start()

    @pl.when(hub)
    def _():
        loop(0, pieces // 2, take_hub)
        loop(0, LEAD, pass_leaf)
        loop(pieces // 2, pieces, take_hub)
        for s in range(slots):
            for g in others + [grp]:
                for k in range(2):
                    x_y(s, g, k).wait_recv()

        def first(j):
            value = dot(xs[grp, 0], wbuf[j, grp, 0])
            for g in others:
                value = value + dot(xs[g, 0], wbuf[j, g, 0])
            acc[j] = value

        loop(0, pieces, first)
        for p in range(2 * slots):
            for d in span:
                for k in range(2):
                    x_z(p, d, k).wait_recv()

    @pl.when(leaf)
    def _():
        for s in range(slots):
            for d in span:
                for k in range(2):
                    x_y(s, others[d], k).wait_recv()
                    x_z(slots + s, d, k).start()

        def send_w(j):
            w_pair(j, 1).start()

        loop(LEAD, pieces, send_w)
        for s in range(slots):
            for k in range(2):
                x_y(s, grp, k).wait_recv()

        def first(j):
            w_pair(j, 0).wait_recv()
            acc[j] = dot(xs[grp, 0], wbuf[j, grp, 0]) + dot(xs[grp, 1], wbuf[j, grp, 1])

        loop(0, pieces, first)
        def second(j):
            value = acc[j]
            if keep:
                for d in span:
                    w_keep(j, d).wait_recv()
                    value = value + dot(
                        xs[others[d], 0, :, 0:keep], wbuf[j, others[d], 0, 0:keep]
                    )
                acc[j] = value
            ys[j] = value[total:].astype(jnp.bfloat16)
            y_copy(j).start()

            @pl.when(rear | ((bit == 0) & (j == final)))
            def _():
                es[j] = value[:total].astype(jnp.bfloat16)
                e_copy(j).start()

        loop(0, pieces, second)

    def send_prior(j):
        @pl.when((me < n - 1) & jnp.logical_not(cross) & jnp.logical_not(rear | (leaf & (bit == 0) & (j == final))))
        def _():
            p_copy(j).start()

    def cross_over(j):
        @pl.when(cross & (j % 2 == 1))
        def _():
            p_copy(j).start()

        @pl.when(relay & (j % 2 == 0))
        def _():
            r_copy(j).start()

    held = pieces - LEAD - 2

    def meet_hub(j, last):
        part = jnp.zeros((2 * total, HEAD), jnp.float32)
        for g in others:
            part = part + dot(lx[g, 0, :, keep:], wbuf[j, g, 0, keep:])
        part_s[...] = part
        acc[j] = acc[j] + dot(xs[grp, 1], wbuf[j, grp, 1])
        for d in span:
            w_hub(j, 1, d, others[d]).wait_recv()
        part = part_s[...]
        for g in others:
            part = part + dot(lx[g, 1], wbuf[j, g, 1])
        if last:
            us[...] = part.astype(jnp.bfloat16)

            @pl.when(bit == 0)
            def _():
                slant(0, 2 * total).start()
                near(total).start()

            @pl.when(bit == 1)
            def _():
                near(2 * total).start()
                slant(total, total).start()
        else:
            ls[j] = part[total:].astype(jnp.bfloat16)
            l_copy(j).start()
        value = acc[j]
        for g in others:
            value = value + dot(xs[g, 1], wbuf[j, g, 1])
        ys[j] = value[total:].astype(jnp.bfloat16)
        y_copy(j).start()
        acc[j, 0:total] = value[:total]
        acc[j, total:] = part[:total]

        @pl.when(mate)
        def _():
            fs[j] = part[:total].astype(jnp.bfloat16)
            f_copy(j).start()

        @pl.when(cross & (j % 2 == 0))
        def _():
            es[j] = value[:total].astype(jnp.bfloat16)
            e_copy(j).start()

        @pl.when(front)
        def _():
            behind[j] = part[total:]

        @pl.when(relay & (j % 2 == 0))
        def _():
            side[j] = value[total:]

    def settle_hub(j, last=False):
        if not last:
            l_copy(j).wait_recv()
            zs[j] = (acc[j, total:] + lr[j].astype(jnp.float32)).astype(jnp.bfloat16)
            z_copy(j).start()
        y_copy(j).wait_recv()
        kv[j] = (acc[j, 0:total] + yr[j].astype(jnp.float32)).astype(jnp.bfloat16)
        send_prior(j)

        @pl.when(relay & (j % 2 == 0))
        def _():
            e_copy(j).wait_recv()
            kx[j] = (side[j] + er[j].astype(jnp.float32)).astype(jnp.bfloat16)

        @pl.when((j < EARLY) | (j > held))
        def _():
            cross_over(j)

        @pl.when(j == held)
        def _():
            loop(EARLY, held + 1, cross_over)

    def gather_leaf(j):
        y_copy(j).wait_recv()
        value = acc[j, 0:total] + yr[j].astype(jnp.float32)
        acc[j, 0:total] = value

        @pl.when((bit == 1) & (j == final))
        def _():
            e_copy(j).wait_recv()
            acc[j, total:] = acc[j, total:] + er[j].astype(jnp.float32)

        @pl.when(base)
        def _():
            e_copy(j).wait_recv()
            kx[j] = (acc[j, total:] + er[j].astype(jnp.float32)).astype(jnp.bfloat16)
            q_copy(j).start()

    def meet_leaf(j):
        z_copy(j).wait_recv()
        kv[j] = (acc[j, 0:total] + zr[j].astype(jnp.float32)).astype(jnp.bfloat16)
        send_prior(j)

    def last_leaf():
        def sums(mine, other):
            value = acc[final, mine:mine + total] + ua[mine:mine + total].astype(jnp.float32)
            return (value + ub[other:other + total].astype(jnp.float32)).astype(jnp.bfloat16)

        @pl.when(bit == 0)
        def _():
            near(total).wait_recv()
            slant(total, total).wait_recv()
            kv[final] = sums(0, 0)

        @pl.when(bit == 1)
        def _():
            near(2 * total).wait_recv()
            slant(0, 2 * total).wait_recv()
            kv[final] = sums(0, total)
            prior[final] = sums(total, 0)

        send_prior(final)

    lane = lax.broadcasted_iota(jnp.int32, (tok, tok), 1)
    own = lane <= lax.broadcasted_iota(jnp.int32, (tok, tok), 0)
    key_pos = lane + jnp.where(own, me, me - 1) * tok
    wide = q_per_kv * HEAD

    def out_copy(h):
        cols = pl.ds(pl.multiple_of(h * wide, HEAD), wide)
        return pltpu.make_async_copy(o_v.at[:, :, cols], o_hbm.at[0, :, :, cols], lo_sem.at[h])

    def wait_prior(j):
        @pl.when((me > 0) & jnp.logical_not(front | (leaf & (bit == 1) & (j == final))))
        def _():
            p_copy(j).wait_recv()

        @pl.when(front)
        def _():
            q_copy(j).wait_recv()
            f_copy(j).wait_recv()
            prior[j] = (
                behind[j] + kq[j].astype(jnp.float32) + fr[j].astype(jnp.float32)
            ).astype(jnp.bfloat16)

    def weigh(h):
        wait_prior(2 * h)
        for s in range(slots):
            here = slice(s * tok, (s + 1) * tok)
            keys = jnp.concatenate([prior[2 * h, here], kv[2 * h, here]], axis=0)
            allowed = key_pos >= start_s[s]
            for q in range(q_per_kv):
                cols = pl.ds(pl.multiple_of((h * q_per_kv + q) * HEAD, HEAD), HEAD)
                both = lax.dot_general(
                    q_v[s, :, cols], keys, (((1,), (1,)), ((), ())),
                    preferred_element_type=jnp.float32,
                )
                scores = jnp.where(own, both[:, tok:], both[:, :tok]) * HEAD ** (-0.5)
                scores = jnp.where(allowed, scores, -1e30)
                maxima = jnp.max(scores, axis=-1, keepdims=True)
                exponent = jnp.exp(scores - maxima)
                sums = jnp.sum(exponent, axis=-1, keepdims=True)
                soft = exponent * (1.0 / sums)
                weights[s, q, :, 0:tok] = jnp.where(own, 0.0, soft).astype(jnp.bfloat16)
                weights[s, q, :, tok:] = jnp.where(own, soft, 0.0).astype(jnp.bfloat16)

    def mix(h):
        wait_prior(2 * h + 1)
        for s in range(slots):
            here = slice(s * tok, (s + 1) * tok)
            values = jnp.concatenate([prior[2 * h + 1, here], kv[2 * h + 1, here]], axis=0)
            for q in range(q_per_kv):
                cols = pl.ds(pl.multiple_of((h * q_per_kv + q) * HEAD, HEAD), HEAD)
                o_v[s, :, cols] = dot(weights[s, q], values).astype(jnp.bfloat16)
        out_copy(h).start()

    @pl.when(hub)
    def _():
        first_late = jnp.where(far, EARLY // 2, heads - LAG)

        def step(j):
            meet_hub(j, False)

            @pl.when(j + LEAD < pieces)
            def _():
                pass_leaf(j + LEAD)

            @pl.when(j > 0)
            def _():
                settle_hub(j - 1)

            @pl.when((j % 2 == 1) & (j > 2 * LAG) & (j // 2 - LAG < first_late))
            def _():
                weigh(j // 2 - LAG)
                mix(j // 2 - LAG)

        loop(0, final, step)

        @pl.when(first_late == heads - LAG)
        def _():
            weigh(heads - 1 - LAG)
            mix(heads - 1 - LAG)

        settle_hub(final - 1)
        meet_hub(final, True)

        @pl.when(far)
        def _():
            weigh(first_late)
            mix(first_late)

        settle_hub(final, True)

        def rest(h):
            weigh(h)
            mix(h)

        loop(first_late + jnp.where(far, 1, 0), heads, rest)

    @pl.when(leaf)
    def _():
        def step(h):
            meet_leaf(2 * h)

            @pl.when(h > 0)
            def _():
                mix(h - 1)

            weigh(h)

            @pl.when(2 * h + 1 < final)
            def _():
                meet_leaf(2 * h + 1)

        loop(0, pieces, gather_leaf)
        loop(0, heads, step)
        last_leaf()
        mix(heads - 1)

    def drain(j):
        y_copy(j).wait_send()

        @pl.when((me < n - 1) & jnp.logical_not(
            (cross & (j % 2 == 0)) | rear | (leaf & (bit == 0) & (j == final))
        ))
        def _():
            p_copy(j).wait_send()

        @pl.when(base)
        def _():
            q_copy(j).wait_send()

        @pl.when(mate)
        def _():
            f_copy(j).wait_send()

        @pl.when((cross & (j % 2 == 0)) | rear | (leaf & (bit == 0) & (j == final)))
        def _():
            e_copy(j).wait_send()

        @pl.when(relay & (j % 2 == 0))
        def _():
            r_copy(j).wait_send()

        @pl.when(hub)
        def _():
            w_pair(j, 0).wait_send()

            @pl.when(j < final)
            def _():
                l_copy(j).wait_send()
                z_copy(j).wait_send()

            for d in span:
                w_hub(j, 0, d, grp).wait_send()
                w_hub(j, 1, d, grp).wait_send()
                if keep:
                    w_keep(j, d).wait_send()

        @pl.when(leaf)
        def _():
            w_pair(j, 1).wait_send()

    loop(0, pieces, drain)

    @pl.when(hub & (bit == 0))
    def _():
        slant(0, 2 * total).wait_send()
        near(total).wait_send()

    @pl.when(hub & (bit == 1))
    def _():
        near(2 * total).wait_send()
        slant(total, total).wait_send()

    for s in range(slots):
        for g in range(groups):
            for k in range(2):
                x_y(s, g, k).wait_send()

    @pl.when(leaf)
    def _():
        for p in range(2 * slots):
            for d in span:
                for k in range(2):
                    x_z(p, d, k).wait_send()

    for h in range(heads):
        out_copy(h).wait()


def body(tokens, queries, gains, key_weight, value_weight, lengths):
    n = lax.axis_size(AXIS)
    _, slots, tok, depth = tokens.shape
    _, rows, key_width = key_weight.shape
    heads = key_width // HEAD
    pieces = 2 * heads
    groups = n // 4
    total = slots * tok
    keep = rows // 2 // HEAD * HEAD
    bf, f32 = jnp.bfloat16, jnp.float32
    any_spec = pl.BlockSpec(memory_space=pl.ANY)
    vmem_spec = pl.BlockSpec(memory_space=pltpu.VMEM)
    dma = pltpu.SemaphoreType.DMA
    fan = groups - 1
    return pl.pallas_call(
        functools.partial(kernel, n, keep),
        out_shape=jax.ShapeDtypeStruct(queries.shape, bf),
        in_specs=[any_spec, any_spec, vmem_spec, any_spec, any_spec, vmem_spec],
        out_specs=any_spec,
        scratch_shapes=[
            pltpu.VMEM((slots, tok, depth), bf),
            pltpu.VMEM(queries.shape[1:], bf),
            pltpu.VMEM(queries.shape[1:], bf),
            pltpu.VMEM((pieces, groups, 2, rows, HEAD), bf),
            pltpu.VMEM((groups, 2, 2 * total, rows), bf),
            pltpu.VMEM((groups, 2, total, rows), bf),
            pltpu.VMEM((groups, 2, 2 * total, rows), bf),
            pltpu.VMEM((pieces, 2 * total, HEAD), f32),
            pltpu.VMEM((pieces, total, HEAD), bf),
            pltpu.VMEM((pieces, total, HEAD), bf),
            pltpu.VMEM((pieces, total, HEAD), bf),
            pltpu.VMEM((pieces, total, HEAD), bf),
            pltpu.VMEM((pieces, total, HEAD), bf),
            pltpu.VMEM((pieces, total, HEAD), bf),
            pltpu.VMEM((pieces, total, HEAD), bf),
            pltpu.VMEM((pieces, total, HEAD), bf),
            pltpu.VMEM((pieces, total, HEAD), bf),
            pltpu.VMEM((pieces, total, HEAD), bf),
            pltpu.VMEM((pieces, total, HEAD), bf),
            pltpu.VMEM((pieces, total, HEAD), bf),
            pltpu.VMEM((pieces, total, HEAD), bf),
            pltpu.VMEM((pieces, total, HEAD), bf),
            pltpu.VMEM((pieces, total, HEAD), f32),
            pltpu.VMEM((pieces, total, HEAD), f32),
            pltpu.VMEM((2 * total, HEAD), f32),
            pltpu.VMEM((2 * total, HEAD), bf),
            pltpu.VMEM((2 * total, HEAD), bf),
            pltpu.VMEM((2 * total, HEAD), bf),
            pltpu.VMEM((slots, queries.shape[-1] // key_width, tok, 2 * tok), bf),
            pltpu.VMEM((slots, tok, HEAD), jnp.int32),
            dma((pieces,)), dma((slots,)), dma, dma((heads,)),
            dma((pieces,)), dma((pieces,)),
            dma((pieces, 2, fan)), dma((pieces, 2, groups)),
            dma((pieces, fan)), dma((pieces, fan)),
            dma((slots, groups, 2)), dma((slots, groups, 2)),
            dma((2 * slots, fan, 2)), dma((2 * slots, fan, 2)),
            dma((pieces,)), dma((pieces,)),
            dma((pieces,)), dma((pieces,)),
            dma((pieces,)), dma((pieces,)),
            dma((pieces,)), dma((pieces,)),
            dma((pieces,)), dma((pieces,)), dma((pieces,)), dma((pieces,)),
            dma((pieces,)), dma((pieces,)), dma((pieces,)),
            dma((2,)), dma((2,)),
        ],
        compiler_params=pltpu.CompilerParams(
            collective_id=0, has_side_effects=True, vmem_limit_bytes=60 * 1024 * 1024
        ),
    )(tokens, queries, gains, key_weight, value_weight, lengths)


def solution(mesh):
    return jax.shard_map(
        body,
        mesh=mesh,
        in_specs=(
            P("section", None, "fsdp", None),
            P("section", None, "fsdp", None),
            P("section", None),
            P("section", "fsdp", None),
            P("section", "fsdp", None),
            P(),
        ),
        out_specs=P("section", None, "fsdp", None),
        check_vma=False,
    )
```
